32 devices in a mesh: req: 2 (over y), patch: 16 (over z, x, core).
Axes of the slice: x: 2, y: 2, z: 4, core: 2. Of those that a mesh axis runs over, the one named last changes fastest.
Arguments:
- tokens: bfloat16 [1536, 1152], P(('req', 'patch')), parts along dimension 0, may hold values from -6 to 6
- positions: int32 [2, 1536], P(None, ('req', 'patch')), parts along dimension 1, may hold values from 0 to 95
- counts: int32 [32], P('req'), parts along dimension 0, may hold values from 1 to 48, 384 in all
- timestep: int32 [2], P('req'), parts along dimension 0, may hold values from 0 to 999
- time_in: bfloat16 [256, 1152], replicated, may hold values from -0.375 to 0.375
- time_out: bfloat16 [1152, 1152], P(None, 'patch'), may hold values from -0.1875 to 0.1875
- ada_weight: bfloat16 [1152, 3456], P('patch'), may hold values from -0.375 to 0.375
- qkv_weight: bfloat16 [1152, 3456], replicated, may hold values from -2 to 2, as said below
- out_weight: bfloat16 [1152, 1152], replicated, may hold values from -0.1875 to 0.1875
Outputs:
- block_out: bfloat16 [1536, 1152], P(('req', 'patch')), parts along dimension 0
The draws below stay inside these ranges and needn't reach their ends.
There are 2 independent parts, one for each index of `req`. The reference program is written for one: setup_inputs(seed, part) draws one part's arguments, and reference() takes and returns one part's arrays. A program takes and returns all parts, laid end to end along the dimension named above; an argument that names none is the same for every part. Nothing has to cross between parts.
Inputs may be any that keep to these rules, and one draw needn't show every extreme that they name: `counts`: used slots are the first ones of each block; they sum to exactly 384, and some block uses all 48. `qkv_weight`: columns are 1152 of queries, 1152 of keys, 1152 of values, each head's 72 columns side by side.
All inputs are finite; a program needn't handle non-finite values.
Results may differ from the reference program's by a relative error of at most 0.0039.
Values may be sent and summed in bfloat16 or wider, within the bound.
A program may use at most 64 MiB of HBM per device.

```python
import math
import jax
import jax.numpy as jnp
import numpy as np
from jax import lax

D = 1152
HEADS = 16
HEAD_DIM = 72
FREQ = 256
TOK_DEV = 48
SLOTS = 768
VALID = 384
N_PATCH = 16


def draw_qkv_weight(key, part):
    base_values = jax.random.truncated_normal(key, -4.0, 4.0, (D, 3 * D), jnp.float32) / math.sqrt(D)
    column_kind = jnp.arange(3 * D) // D
    scaled = base_values * jnp.where(column_kind < 2, 1.3, 1.0)[None, :]
    return jnp.clip(scaled, -2.0, 2.0).astype(jnp.bfloat16)


def set_ends(values, stream_key, low, high):
    place = [jax.random.randint(jax.random.fold_in(stream_key, axis), (), 0, length) for axis, length in enumerate(values.shape)]
    widest = values.shape.index(max(values.shape))
    neighbour = place[:widest] + [(place[widest] + 1) % values.shape[widest]] + place[widest + 1:]
    return values.at[tuple(place)].set(low).at[tuple(neighbour)].set(high)


def level_of(key, shape, split, smallest, top_value):
    def one(position, blocks):
        draws = jax.random.uniform(jax.random.fold_in(jax.random.fold_in(key, 6), position), (blocks,), jnp.float32, smallest / len(split), top_value / len(split))
        return jnp.repeat(jnp.exp(draws), shape[position] // blocks).reshape((-1,) + (1,) * (len(shape) - position - 1))

    gain = one(*split[0])
    for cut in split[1:]:
        gain = gain * one(*cut)
    return gain


def length_profile(number_of, total, reach, skew):
    portions = [(1 << 20) // math.isqrt(standing ** skew) + 1 for standing in range(2, number_of + 1)]
    spare, holding = total - reach - (number_of - 1), [1] * (number_of - 1)
    while spare > 0:
        movable = [i for i in range(number_of - 1) if holding[i] < reach]
        mass, budget = sum([portions[i] for i in movable]), spare
        for i in movable:
            extra = min(reach - holding[i], max(1, budget * portions[i] // mass), spare)
            holding[i] = holding[i] + extra
            spare = spare - extra
    return np.array([reach] + holding)


def uneven_parts(key, count, total, most, skew):
    if count == 2:
        one = jax.random.randint(key, (), max(1, total - most), min(most, total - 1) + 1)
        return jnp.stack([one, total - one])
    tallies = jnp.asarray(length_profile(count, total, most, skew), jnp.int32)
    pairs = (count - 1) // 2
    donor, sink = tallies[1:1 + 2 * pairs:2], tallies[2:2 + 2 * pairs:2]
    room = jnp.minimum(donor - 1, most - sink)
    moved = jax.random.randint(jax.random.fold_in(key, 1), (pairs,), 0, 1 << 20) % (room + 1)
    tallies = tallies.at[1:1 + 2 * pairs:2].set(donor - moved).at[2:2 + 2 * pairs:2].set(sink + moved)
    return tallies[jax.random.permutation(jax.random.fold_in(key, 2), count)]


def noise(key, shape, deviation, reach, pieces=(), kind=jnp.bfloat16):
    loudness = level_of(key, shape, pieces, -0.22, 0.18) if pieces else 1.0
    drawn = jax.random.normal(key, shape, jnp.float32) * deviation * loudness
    return jnp.minimum(jnp.maximum(drawn, -reach), reach).astype(kind)


def setup_inputs(seed: int = 0, part: int = 0) -> dict:
    streams_of = jax.random.split(jax.random.key(seed), 10)
    own_keys = jax.random.split(jax.random.fold_in(streams_of[9], part), 10)
    tokens = noise(own_keys[0], (SLOTS, D), 1.0, 6.0, ((0, 16),))
    positions = set_ends(jax.random.randint(own_keys[1], (2, SLOTS), 0, 96), jax.random.fold_in(own_keys[1], 1), 0, 95).astype(jnp.int32)
    counts = uneven_parts(own_keys[2], N_PATCH, VALID, TOK_DEV, 2).astype(jnp.int32)
    timestep = jax.random.randint(own_keys[3], (1,), 0, 1000).astype(jnp.int32)
    time_in = noise(streams_of[4], (FREQ, D), FREQ ** -0.5, 0.375)
    time_out = noise(streams_of[5], (D, D), D ** -0.5, 0.1875, ((1, 16),))
    ada_weight = noise(streams_of[6], (D, 3 * D), (D // 4) ** -0.5, 0.375, ((0, 16),))
    qkv_weight = draw_qkv_weight(jax.random.fold_in(streams_of[9], 71), part)
    out_weight = noise(streams_of[8], (D, D), D ** -0.5, 0.1875)
    return dict(tokens=tokens, positions=positions, counts=counts, timestep=timestep, time_in=time_in, time_out=time_out, ada_weight=ada_weight, qkv_weight=qkv_weight, out_weight=out_weight)


def time_features(timestep, freq_size):
    half_size = freq_size // 2
    frequencies = jnp.exp(-math.log(10000.0) * jnp.arange(half_size, dtype=jnp.float32) / half_size)
    angles = timestep.astype(jnp.float32)[:, None] * frequencies[None, :]
    return jnp.concatenate([jnp.cos(angles), jnp.sin(angles)], axis=1).astype(jnp.bfloat16)

def position_table(positions, model_width):
    quarter = model_width // 4
    omegas = jnp.power(10000.0, -jnp.arange(quarter, dtype=jnp.float32) / quarter)
    row_angle = positions[0].astype(jnp.float32)[:, None] * omegas[None, :]
    col_angle = positions[1].astype(jnp.float32)[:, None] * omegas[None, :]
    return jnp.concatenate([jnp.sin(row_angle), jnp.cos(row_angle), jnp.sin(col_angle), jnp.cos(col_angle)], axis=1)

def reference(tokens, positions, counts, timestep, time_in, time_out, ada_weight, qkv_weight, out_weight):
    model_width = tokens.shape[1]
    slot_count = tokens.shape[0]
    per_device = slot_count // N_PATCH
    features = time_features(timestep, FREQ)
    hidden_time = jax.nn.silu(jnp.dot(features, time_in, preferred_element_type=jnp.float32)).astype(jnp.bfloat16)
    cond = jnp.dot(hidden_time, time_out, preferred_element_type=jnp.float32)
    activated = jax.nn.silu(cond).astype(jnp.bfloat16)
    modulation = jnp.dot(activated, ada_weight, preferred_element_type=jnp.float32)
    shift_mod = modulation[:, :model_width]
    scale_mod = modulation[:, model_width:2 * model_width]
    gate_mod = modulation[:, 2 * model_width:]
    x_in = tokens.astype(jnp.float32) + position_table(positions, model_width)
    mean_value = lax.optimization_barrier(jnp.mean(x_in, axis=1, keepdims=True))
    centered = x_in - mean_value
    variance = lax.optimization_barrier(jnp.mean(centered * centered, axis=1, keepdims=True))
    normed = centered * lax.rsqrt(variance + 1e-06)
    modulated = (normed * (1.0 + scale_mod) + shift_mod).astype(jnp.bfloat16)
    projections = jnp.dot(modulated, qkv_weight, preferred_element_type=jnp.float32).astype(jnp.bfloat16)
    slot_valid = (jnp.arange(per_device, dtype=jnp.int32)[None, :] < counts[:, None]).reshape(slot_count)
    key_heads = projections[:, model_width:2 * model_width].astype(jnp.float32).reshape(slot_count, HEADS, HEAD_DIM)
    value_heads = projections[:, 2 * model_width:].astype(jnp.float32).reshape(slot_count, HEADS, HEAD_DIM)
    query_blocks = projections[:, :model_width].astype(jnp.float32).reshape(N_PATCH, per_device, HEADS, HEAD_DIM)
    inv_root = 1.0 / math.sqrt(HEAD_DIM)

    def attend(query_block):
        scores = jnp.einsum('qhd,khd->hqk', query_block, key_heads, precision=lax.Precision.HIGHEST) * inv_root
        scores = jnp.where(slot_valid[None, None, :], scores, -1e+30)
        row_top = lax.optimization_barrier(jnp.max(scores, axis=2, keepdims=True))
        weights = jnp.where(slot_valid[None, None, :], jnp.exp(scores - row_top), 0.0)
        denominator = lax.optimization_barrier(jnp.sum(weights, axis=2, keepdims=True))
        rounded = lax.optimization_barrier(weights.astype(jnp.bfloat16))
        weighted = jnp.einsum('hqk,khd->qhd', rounded.astype(jnp.float32), value_heads, precision=lax.Precision.HIGHEST)
        return weighted / jnp.transpose(denominator, (1, 0, 2))
    attended = lax.map(attend, query_blocks).reshape(slot_count, model_width).astype(jnp.bfloat16)
    projected = jnp.dot(attended, out_weight, preferred_element_type=jnp.float32)
    valid_column = slot_valid.astype(jnp.float32)[:, None]
    return (x_in + gate_mod * projected * valid_column).astype(jnp.bfloat16)
```

```python
import functools
import math

import jax
import jax.numpy as jnp
import numpy as np
from jax import lax
from jax.experimental import pallas as pl
from jax.experimental.pallas import tpu as pltpu
from jax.sharding import PartitionSpec as P

HEADS = 16
NEG = -1e30
F32 = jnp.float32
BF16 = jnp.bfloat16
MESH = pl.DeviceIdType.MESH


def silu(v):
    return v / (1.0 + jnp.exp(-v))


def dot(a, b):
    return jnp.dot(a, b, preferred_element_type=F32)


def one_row_dot(row, matrix):
    wide = jnp.broadcast_to(row, (16, row.shape[1])).astype(BF16)
    return dot(wide, matrix)[0:1]


def fold_group(rows, extra):
    group = 8
    while rows // group * extra > 128:
        group *= 2
    return group


def fold(block):
    rows, extra = block.shape[0], block.shape[1] - 64
    group = fold_group(rows, extra)
    half = rows // 2
    main = jnp.concatenate([block[:half, :64], block[half:, :64]], axis=1)
    pieces = [block[r : r + group, 64:] for r in range(0, rows, group)]
    spare = 128 - extra * len(pieces)
    rest = jnp.concatenate(pieces + [jnp.zeros((group, spare), F32)], axis=1)
    return jnp.concatenate([main, rest], axis=0)


def unfold(packed, rows, extra):
    half = rows // 2
    left = jnp.concatenate([packed[:half, :64], packed[:half, 64:]], axis=0)
    rest = packed[half:]
    count = rows // fold_group(rows, extra)
    right = jnp.concatenate([rest[:, r * extra : (r + 1) * extra] for r in range(count)], axis=0)
    return jnp.concatenate([left, right], axis=1)


def block_kernel(
    n, rows, width, head,
    counts_h, tstep_h, pos_h, pos_tab_h, time_tab_h,
    tok_h, tin_h, tout_h, ada_h, qkv_h, ow_h,
    out,
    counts, tstep, pos, pos_tab, time_tab, tok, tin, tout, ada, qkv, ow, mods, gates, xin_s, norm_s, send, got, kbuf, vbuf, att, back,
    lsem, ssem, wsem, msend, mrecv, gsend, grecv, psend, precv, asend, arecv,
):
    me = lax.axis_index("patch")
    my_head = lax.rem(me, HEADS)
    group = me // HEADS
    chunk = HEADS * rows
    groups = n // HEADS
    inv_root = math.log2(math.e) / math.sqrt(head)

    barrier = pltpu.get_barrier_semaphore()

    def drain(ref, sem):
        pltpu.make_async_copy(ref, ref, sem.at[0]).wait()

    @pl.loop(1, n)
    def _(step):
        pl.semaphore_signal(
            barrier, inc=1, device_id={"patch": lax.rem(me + step, n)}, device_id_type=MESH
        )

    loads = [
        pltpu.make_async_copy(src, dst, lsem.at[i])
        for i, (src, dst) in enumerate(
            [(tin_h, tin), (tout_h, tout), (ada_h, ada), (tok_h, tok), (qkv_h, qkv)]
        )
    ]
    small = [
        pltpu.make_async_copy(src, dst, ssem.at[i])
        for i, (src, dst) in enumerate(
            [(tstep_h, tstep), (time_tab_h, time_tab), (counts_h, counts),
             (pos_h, pos), (pos_tab_h, pos_tab)]
        )
    ]
    for load in small[:2] + loads[:4] + small[2:]:
        load.start()
    for load in small[:2]:
        load.wait()

    angles = tstep[0].astype(F32) * time_tab[0:1, :] + time_tab[1:2, :]
    features = jnp.sin(angles).astype(BF16)
    loads[0].wait()
    hidden = silu(one_row_dot(features, tin[...])).astype(BF16)
    loads[1].wait()
    wide = jnp.broadcast_to(hidden, (16, width))
    cond = lax.dot_general(wide, tout[...], (((1,), (1,)), ((), ())), preferred_element_type=F32)
    activated = silu(cond[0:1]).astype(BF16)
    loads[2].wait()
    partial = one_row_dot(activated, ada[...])
    mods[me] = jnp.concatenate(
        [partial[:, :width], partial[:, width : 2 * width]], axis=0
    ).astype(BF16)
    span = gates.shape[2]
    gates[me] = jnp.concatenate(
        [partial[:, 2 * width : 2 * width + span], partial[:, 3 * width - span :]], axis=0
    ).astype(BF16)
    loads[4].start()

    pl.semaphore_wait(barrier, n - 1)

    def mod_copy(step, slot):
        return pltpu.make_async_remote_copy(
            src_ref=mods.at[slot],
            dst_ref=mods.at[slot],
            send_sem=msend.at[0],
            recv_sem=mrecv.at[0],
            device_id={"patch": lax.rem(me + step, n)},
            device_id_type=MESH,
        )

    def gate_copy(step, slot):
        return pltpu.make_async_remote_copy(
            src_ref=gates.at[slot],
            dst_ref=gates.at[slot],
            send_sem=gsend.at[0],
            recv_sem=grecv.at[0],
            device_id={"patch": lax.rem(me + step, n)},
            device_id_type=MESH,
        )

    @pl.loop(1, n)
    def _(step):
        mod_copy(step, me).start()

    ow[:, head:, :] = jnp.zeros((HEADS, ow.shape[1] - head, width), BF16)
    ow_loads = [
        pltpu.make_async_copy(
            ow_h.at[pl.ds(h * head, head), :], ow.at[h, pl.ds(0, head), :], wsem.at[0]
        )
        for h in range(HEADS)
    ]
    for load in ow_loads:
        load.start()

    ids = lax.broadcasted_iota(jnp.int32, (rows, rows), 0)
    eye = ids == lax.broadcasted_iota(jnp.int32, (rows, rows), 1)
    for load in small[2:]:
        load.wait()
    posf = pos[...].astype(F32)
    row_col = jnp.sum(jnp.where(eye, posf[0:1, :], 0.0), axis=1, keepdims=True)
    col_col = jnp.sum(jnp.where(eye, posf[1:2, :], 0.0), axis=1, keepdims=True)
    lanes = lax.broadcasted_iota(jnp.int32, (1, width), 1)
    first = lanes < width // 2
    place = jnp.where(first, row_col, col_col)
    embed = jnp.sin(place * pos_tab[0:1, :] + pos_tab[1:2, :])
    loads[3].wait()
    x_in = tok[...].astype(F32) + embed
    xin_s[...] = x_in
    centered = x_in - jnp.mean(x_in, axis=1, keepdims=True)
    variance = jnp.mean(centered * centered, axis=1, keepdims=True)
    norm_s[...] = centered * lax.rsqrt(variance + 1e-6)

    drain(mods.at[pl.ds(0, n - 1)], mrecv)

    @pl.loop(1, n)
    def _(step):
        gate_copy(step, me).start()

    modulation = jnp.sum(mods[...].astype(F32), axis=0)
    shift = modulation[0:1]
    scale = modulation[1:2]
    modulated = (norm_s[...] * (1.0 + scale) + shift).astype(BF16)
    loads[4].wait()
    spare = jnp.zeros((rows, send.shape[2] - 3 * head), BF16)
    part_heads = HEADS // 2

    def pair_copy(to, slot):
        return pltpu.make_async_remote_copy(
            src_ref=send.at[lax.rem(to, HEADS)],
            dst_ref=got.at[slot],
            send_sem=psend.at[0],
            recv_sem=precv.at[0],
            device_id={"patch": to},
            device_id_type=MESH,
        )

    def make_half(half):
        low = half * part_heads * head
        start = low // 128 * 128
        stop = -(-(low + part_heads * head) // 128) * 128
        parts = [
            dot(modulated, qkv[:, i * width + start : i * width + stop]).astype(BF16)
            for i in range(3)
        ]
        for h in range(part_heads):
            cols = slice(low - start + h * head, low - start + (h + 1) * head)
            send[half * part_heads + h] = jnp.concatenate(
                [part[:, cols] for part in parts] + [spare], axis=1
            )

        @pl.loop(0, groups * part_heads)
        def _(j):
            turn = lax.rem(me + j, part_heads)
            to = (j // part_heads) * HEADS + half * part_heads + turn

            @pl.when(to != me)
            def _():
                pair_copy(to, me).start()

    @pl.when(my_head < part_heads)
    def _():
        make_half(1)
        make_half(0)

    @pl.when(my_head >= part_heads)
    def _():
        make_half(0)
        make_half(1)

    got[me] = send[my_head]
    tail = lax.broadcasted_iota(jnp.int32, (chunk, vbuf.shape[1] - head), 1)
    ones = jnp.where(tail == 0, 1.0, 0.0).astype(BF16)
    slot_ids = lax.broadcasted_iota(jnp.int32, (rows, 1), 0)
    lane_ids = lax.broadcasted_iota(jnp.int32, (rows, kbuf.shape[1]), 1)
    for g in range(groups):
        vbuf[g * chunk : (g + 1) * chunk, head:] = ones
    for b in range(n):
        bias = jnp.where(slot_ids < counts[b], 0.0, NEG)
        kbuf[b * rows : (b + 1) * rows, :] = jnp.where(lane_ids == head, bias, 0.0).astype(BF16)

    drain(got.at[pl.ds(0, n - 1)], precv)

    for g in range(groups):
        block = got[g * HEADS : (g + 1) * HEADS].reshape(chunk, got.shape[2])
        kbuf[g * chunk : (g + 1) * chunk, :head] = block[:, head : 2 * head]
        vbuf[g * chunk : (g + 1) * chunk, :head] = block[:, 2 * head : 3 * head]


    def att_copy(j, slot, to):
        return pltpu.make_async_remote_copy(
            src_ref=att.at[j],
            dst_ref=back.at[slot],
            send_sem=asend.at[0],
            recv_sem=arecv.at[0],
            device_id={"patch": group * HEADS + to},
            device_id_type=MESH,
        )

    pairs = HEADS // 4
    mine = my_head // pairs

    @pl.loop(0, HEADS // pairs)
    def _(step):
        base = lax.rem(mine // 2 + 1 + step // 2, 2) * 2 + lax.rem(mine + 1 + step, 2)
        base = base * pairs
        block = got[pl.ds(group * HEADS + base, pairs)].reshape(pairs * rows, got.shape[2])
        query = jnp.concatenate(
            [block[:, :head], jnp.ones((pairs * rows, 1), BF16)], axis=1
        )
        query = jnp.concatenate(
            [query, jnp.zeros((pairs * rows, kbuf.shape[1] - head - 1), BF16)], axis=1
        )
        top = weighted = None
        for g in range(groups):
            keys = kbuf[g * chunk : (g + 1) * chunk, :]
            scores = lax.dot_general(
                query, keys, (((1,), (1,)), ((), ())), preferred_element_type=F32
            )
            new_top = jnp.max(scores, axis=1, keepdims=True)
            if g:
                new_top = jnp.maximum(top, new_top)
            prob = jnp.exp2((scores - new_top) * inv_root).astype(BF16)
            mixed = dot(prob, vbuf[g * chunk : (g + 1) * chunk, :])
            if g:
                mixed = weighted * jnp.exp2((top - new_top) * inv_root) + mixed
            top, weighted = new_top, mixed
        total = weighted[:, head : head + 1]
        result = weighted / total
        for i in range(pairs):
            att[base + i] = fold(result[i * rows : (i + 1) * rows, :head]).astype(BF16)
        for i in range(pairs):

            @pl.when(base + i != my_head)
            def _():
                att_copy(base + i, my_head, base + i).start()

    back[my_head] = att[my_head]
    filler = jnp.zeros((rows, ow.shape[1] - head), F32)
    pltpu.make_async_copy(ow_h, ow_h, wsem.at[0]).wait()

    drain(gates.at[pl.ds(0, n - 1)], grecv)

    gate_rows = jnp.sum(gates[...].astype(F32), axis=0)
    gate = jnp.concatenate([gate_rows[0:1], gate_rows[1:2, 2 * span - width :]], axis=1)

    drain(mods.at[pl.ds(0, n - 1)], msend)
    drain(gates.at[pl.ds(0, n - 1)], gsend)
    drain(got.at[pl.ds(0, n - 1)], psend)
    drain(back.at[pl.ds(0, HEADS - 1)], arecv)

    attended = jnp.concatenate(
        [
            piece
            for h in range(HEADS)
            for piece in (unfold(back[h].astype(F32), rows, head - 64), filler)
        ],
        axis=1,
    ).astype(BF16)
    weight = ow[...].reshape(HEADS * ow.shape[1], width)
    valid = (lax.broadcasted_iota(jnp.int32, (rows, 1), 0) < counts[me]).astype(F32)
    cut = width // 256 * 128
    for i, cols in enumerate([slice(0, cut), slice(cut, width)]):
        projected = dot(attended, weight[:, cols])
        out[:, cols] = (xin_s[:, cols] + gate[:, cols] * projected * valid).astype(BF16)

    drain(back.at[pl.ds(0, HEADS - 1)], asend)


def tables(width, freq):
    quarter, half = width // 4, freq // 2
    omega = np.power(10000.0, -np.arange(quarter) / quarter)
    turn = math.pi / 2
    pos_tab = np.stack([np.tile(omega, 4), np.repeat([0.0, turn, 0.0, turn], quarter)])
    wave = np.exp(-math.log(10000.0) * np.arange(half) / half)
    time_tab = np.stack([np.tile(wave, 2), np.repeat([turn, 0.0], half)])
    return pos_tab.astype(np.float32), time_tab.astype(np.float32)


def per_device(
    tokens, positions, counts, timestep, time_in, time_out, ada_weight, qkv_weight, out_weight
):
    n = lax.axis_size("patch")
    rows, width = tokens.shape
    head = width // HEADS
    lane = 128
    head_pad = -(-head // lane) * lane
    pack = -(-3 * head // lane) * lane
    fold_back = rows // 2 + fold_group(rows, head - 64)
    pos_tab, time_tab = tables(width, time_in.shape[0])
    smem = pl.BlockSpec(memory_space=pltpu.SMEM)
    vmem = pl.BlockSpec(memory_space=pltpu.VMEM)
    hbm = pl.BlockSpec(memory_space=pl.ANY)
    result = pl.pallas_call(
        functools.partial(block_kernel, n, rows, width, head),
        out_shape=pltpu.VMEM((rows, width), BF16),
        in_specs=[hbm] * 11,
        out_specs=vmem,
        scratch_shapes=[
            pltpu.SMEM(counts.shape, jnp.int32),
            pltpu.SMEM(timestep.shape, jnp.int32),
            pltpu.VMEM(positions.shape, jnp.int32),
            pltpu.VMEM(pos_tab.shape, F32),
            pltpu.VMEM(time_tab.shape, F32),
            pltpu.VMEM(tokens.shape, BF16),
            pltpu.VMEM(time_in.shape, BF16),
            pltpu.VMEM(time_out.shape[::-1], BF16),
            pltpu.VMEM(ada_weight.shape, BF16),
            pltpu.VMEM(qkv_weight.shape, BF16),
            pltpu.VMEM((HEADS, head_pad, width), BF16),
            pltpu.VMEM((n, 2, width), BF16),
            pltpu.VMEM((n, 2, -(-width // 256) * 128), BF16),
            pltpu.VMEM((rows, width), F32),
            pltpu.VMEM((rows, width), F32),
            pltpu.VMEM((HEADS, rows, pack), BF16),
            pltpu.VMEM((n, rows, pack), BF16),
            pltpu.VMEM((n * rows, head_pad), BF16),
            pltpu.VMEM((n * rows, head_pad), BF16),
            pltpu.VMEM((HEADS, fold_back, lane), BF16),
            pltpu.VMEM((HEADS, fold_back, lane), BF16),
            pltpu.SemaphoreType.DMA((5,)),
            pltpu.SemaphoreType.DMA((5,)),
            pltpu.SemaphoreType.DMA((1,)),
            pltpu.SemaphoreType.DMA((1,)),
            pltpu.SemaphoreType.DMA((1,)),
            pltpu.SemaphoreType.DMA((1,)),
            pltpu.SemaphoreType.DMA((1,)),
            pltpu.SemaphoreType.DMA((1,)),
            pltpu.SemaphoreType.DMA((1,)),
            pltpu.SemaphoreType.DMA((1,)),
            pltpu.SemaphoreType.DMA((1,)),
        ],
        compiler_params=pltpu.CompilerParams(
            collective_id=0, has_side_effects=True, vmem_limit_bytes=60 * 2**20
        ),
    )(
        counts, timestep, positions, pos_tab, time_tab,
        tokens, time_in, time_out.T, ada_weight, qkv_weight, out_weight,
    )
    return result


def solution(mesh):
    placed = (
        P(("req", "patch"), None),
        P(None, ("req", "patch")),
        P("req"),
        P("req"),
        P(),
        P(None, "patch"),
        P("patch", None),
        P(),
        P(),
    )
    return jax.shard_map(
        per_device, mesh=mesh, in_specs=placed, out_specs=P(("req", "patch"), None), check_vma=False
    )
```

```python
import functools
import math

import jax
import jax.numpy as jnp
import numpy as np
from jax import lax
from jax.experimental import pallas as pl
from jax.experimental.pallas import tpu as pltpu
from jax.sharding import PartitionSpec as P

HEADS = 16
PAIRS = HEADS // 2
LANE = 128
NEG = -1e30
F32 = jnp.float32
BF16 = jnp.bfloat16
MESH = pl.DeviceIdType.MESH
PI_PARTS = (3.140625, 0.000967502593994140625, 1.509957990978376432e-07)


def silu(v):
    return v / (1.0 + jnp.exp(-v))


def sine(x):
    turns = jnp.floor(x * (1.0 / math.pi) + 0.5)
    r = x - turns * PI_PARTS[0]
    r = r - turns * PI_PARTS[1]
    r = r - turns * PI_PARTS[2]
    s = r * r
    poly = -2.3889859e-08 * s + 2.7525562e-06
    poly = poly * s - 0.00019840874
    poly = poly * s + 0.0083333310
    poly = poly * s - 0.16666667
    value = r + r * (s * poly)
    odd = turns - 2.0 * jnp.floor(turns * 0.5)
    return value * (1.0 - 2.0 * odd)


def dot(a, b):
    return jnp.dot(a, b, preferred_element_type=F32)


def dot_t(a, b):
    return lax.dot_general(a, b, (((1,), (1,)), ((), ())), preferred_element_type=F32)


def one_row_dot(row, matrix):
    wide = jnp.broadcast_to(row, (16, row.shape[1])).astype(BF16)
    return dot(wide, matrix)[0:1]


def fold_rows(rows, stride):
    group = 8
    while rows % group or rows // group * stride > LANE:
        group += 8
    return group


def turned(x, shift):
    shift %= LANE
    return pltpu.roll(x, shift, axis=1) if shift else x


def fold(blocks, base, group, stride, ex, at):
    lanes = lax.broadcasted_iota(jnp.int32, (group, LANE), 1)
    packed = base
    for r in range(blocks[0].shape[0] // group):
        for j, block in enumerate(blocks):
            low = r * stride + j * ex
            piece = turned(block[r * group : (r + 1) * group], low - at)
            packed = jnp.where((lanes >= low) & (lanes < low + ex), piece, packed)
    return packed


def unfold(packed, rows, stride, to):
    group = packed.shape[0]
    return jnp.concatenate(
        [turned(packed, to - r * stride) for r in range(rows // group)], axis=0
    )


def block_kernel(
    n, rows, width, head,
    counts_h, tstep_h, pos_h, pos_tab_h, time_tab_h,
    tok_h, tin_h, tout_h, ada_h, qkv_h, ow_h,
    out,
    counts, tstep, pos, pos_tab, time_tab, tok, tin, tout, ada, qkv, ow, mods, gates,
    xin_s, norm_s, nsend, ngot, send0, send1, got0, got1, o_s, top_s, att, back,
    lsem, ssem, wsem, msend, mrecv, gsend, grecv, nsem, nrecv, psend, precv, rsend, rrecv,
    asend, arecv,
):
    me = lax.axis_index("patch")
    pair = lax.rem(me, PAIRS)
    side = lax.rem(me // PAIRS, 2)
    group = me // HEADS
    groups = n // HEADS
    mirror = me + PAIRS * (1 - 2 * side)
    ex = 2 * head - LANE
    stride0, stride1 = 3 * ex + 2, 2 * ex + 2
    fold0, fold1, fold2 = fold_rows(rows, stride0), fold_rows(rows, stride1), fold_rows(rows, ex)
    scale_q = math.log2(math.e) / math.sqrt(head)

    barrier = pltpu.get_barrier_semaphore()

    def drain(ref, sem):
        pltpu.make_async_copy(ref, ref, sem.at[0]).wait()

    def remote(src, dst, send, recv, to):
        return pltpu.make_async_remote_copy(
            src_ref=src, dst_ref=dst, send_sem=send.at[0], recv_sem=recv.at[0],
            device_id={"patch": to}, device_id_type=MESH,
        )

    @pl.loop(1, n)
    def _(step):
        pl.semaphore_signal(
            barrier, inc=1, device_id={"patch": lax.rem(me + step, n)}, device_id_type=MESH
        )

    loads = [
        pltpu.make_async_copy(src, dst, lsem.at[i])
        for i, (src, dst) in enumerate(
            [(tin_h, tin), (tout_h, tout), (ada_h, ada), (tok_h, tok), (qkv_h, qkv)]
        )
    ]
    small = [
        pltpu.make_async_copy(src, dst, ssem.at[i])
        for i, (src, dst) in enumerate(
            [(tstep_h, tstep), (time_tab_h, time_tab), (counts_h, counts),
             (pos_h, pos), (pos_tab_h, pos_tab)]
        )
    ]
    for load in small[:2] + loads[:4] + small[2:]:
        load.start()
    for load in small[:2]:
        load.wait()

    angles = tstep[0].astype(F32) * time_tab[0:1, :] + time_tab[1:2, :]
    features = sine(angles).astype(BF16)
    loads[0].wait()
    hidden = silu(one_row_dot(features, tin[...])).astype(BF16)
    loads[1].wait()
    wide = jnp.broadcast_to(hidden, (16, width))
    cond = dot_t(wide, tout[...])
    activated = silu(cond[0:1]).astype(BF16)
    loads[2].wait()
    partial = one_row_dot(activated, ada[...])
    mods[me] = jnp.concatenate(
        [partial[:, :width], partial[:, width : 2 * width]], axis=0
    ).astype(BF16)
    span = gates.shape[2]
    gates[me] = jnp.concatenate(
        [partial[:, 2 * width : 2 * width + span], partial[:, 3 * width - span :]], axis=0
    ).astype(BF16)
    loads[4].start()
    ow_load = pltpu.make_async_copy(ow_h, ow, wsem.at[0])
    ow_load.start()

    pl.semaphore_wait(barrier, n - 1)

    @pl.loop(1, n)
    def _(step):
        remote(mods.at[me], mods.at[me], msend, mrecv, lax.rem(me + step, n)).start()

    ids = lax.broadcasted_iota(jnp.int32, (rows, rows), 0)
    eye = ids == lax.broadcasted_iota(jnp.int32, (rows, rows), 1)
    for load in small[2:]:
        load.wait()
    posf = pos[...].astype(F32)
    row_col = jnp.sum(jnp.where(eye, posf[0:1, :], 0.0), axis=1, keepdims=True)
    col_col = jnp.sum(jnp.where(eye, posf[1:2, :], 0.0), axis=1, keepdims=True)
    wide_lanes = lax.broadcasted_iota(jnp.int32, (1, width), 1)
    place = jnp.where(wide_lanes < width // 2, row_col, col_col)
    embed = sine(place * pos_tab[0:1, :] + pos_tab[1:2, :])
    loads[3].wait()
    x_in = tok[...].astype(F32) + embed
    xin_s[...] = x_in
    centered = x_in - jnp.mean(x_in, axis=1, keepdims=True)
    variance = jnp.mean(centered * centered, axis=1, keepdims=True)
    norm = centered * lax.rsqrt(variance + 1e-6)
    norm_s[...] = norm
    nsend[...] = norm.astype(BF16)
    mirror_copy = remote(nsend, ngot, nsem, nrecv, mirror)
    mirror_copy.start()

    drain(mods.at[pl.ds(0, n - 1)], mrecv)
    modulation = jnp.sum(mods[...].astype(F32), axis=0)
    shift = modulation[0:1]
    gain = 1.0 + modulation[1:2]
    modulated = (norm_s[...] * gain + shift).astype(BF16)
    loads[4].wait()

    lane_ids = lax.broadcasted_iota(jnp.int32, (rows, LANE), 1)

    def base_of(owner, fold_group, stride, blocks):
        lanes = lax.broadcasted_iota(jnp.int32, (fold_group, LANE), 1)
        slot = lax.broadcasted_iota(jnp.int32, (fold_group, LANE), 0)
        base = jnp.zeros((fold_group, LANE), F32)
        for r in range(rows // fold_group):
            low = r * stride + blocks * ex
            base = jnp.where(lanes == low, 1.0, base)
            bias = jnp.where(slot + r * fold_group < counts[owner], 0.0, NEG)
            base = jnp.where(lanes == low + 1, bias, base)
        return base

    def project(first, x):
        return [dot(x, qkv[:, i * width : (i + 1) * width]) for i in range(first, 3)]

    def pack(parts, base, fold_group, stride, buffer):
        for p in range(PAIRS):
            low, cut = p * LANE, p * ex
            nexts = []
            for j, part in enumerate(parts):
                here = part[:, low : low + LANE]
                after = part[:, low + LANE : low + 2 * LANE]
                nexts.append(after)
                mixed = jnp.where(lane_ids < cut, after, here) if cut else here
                buffer[p, j * rows : (j + 1) * rows, :] = mixed.astype(BF16)
            packed = fold(nexts, base, fold_group, stride, ex, cut)
            buffer[p, len(parts) * rows :, :] = packed.astype(BF16)

    def spread(buffer, got, send, recv):
        slot = group * PAIRS + pair

        @pl.loop(1, groups * PAIRS)
        def _(j):
            turn = lax.rem(slot + j, groups * PAIRS)
            to = turn // PAIRS * HEADS + side * PAIRS + lax.rem(turn, PAIRS)
            remote(buffer.at[lax.rem(turn, PAIRS)], got.at[slot], send, recv, to).start()

        got[slot] = buffer[pair]

    parts = project(0, modulated)
    pack([parts[0] * scale_q] + parts[1:], base_of(me, fold0, stride0, 3), fold0, stride0, send0)
    spread(send0, got0, psend, precv)

    @pl.loop(1, n)
    def _(step):
        remote(gates.at[me], gates.at[me], gsend, grecv, lax.rem(me + step, n)).start()

    mirror_copy.wait_recv()
    modulated = (ngot[...].astype(F32) * gain + shift).astype(BF16)
    pack(project(1, modulated), base_of(mirror, fold1, stride1, 2), fold1, stride1, send1)
    spread(send1, got1, rsend, rrecv)

    slots = groups * PAIRS
    drain(got0.at[pl.ds(0, slots - 1)], precv)

    def keys_of(got, g, first, fold_group, stride, to):
        block = got[g * PAIRS : (g + 1) * PAIRS]
        cells = PAIRS * rows
        k = block[:, first * rows : (first + 1) * rows].reshape(cells, LANE)
        v = block[:, (first + 1) * rows : (first + 2) * rows].reshape(cells, LANE)
        extra = jnp.concatenate(
            [unfold(block[s, (first + 2) * rows :].astype(F32), rows, stride, to) for s in range(PAIRS)],
            axis=0,
        ).astype(BF16)
        return jnp.concatenate([k, extra], axis=1), jnp.concatenate([v, extra], axis=1)

    half = PAIRS // 2
    cells = half * rows
    near = pair // half
    q_lanes = lax.broadcasted_iota(jnp.int32, (cells, LANE), 1)
    column = lax.rem(q_lanes + (LANE - ex * pair), LANE)
    first_head = column < head
    bias_one = jnp.where(q_lanes == 3 * ex + 1, 1.0, 0.0)

    def queries_of(base):
        block = got0[pl.ds(group * PAIRS + base, half)]
        qa = block[:, :rows].reshape(cells, LANE).astype(F32)
        extra = jnp.concatenate(
            [
                unfold(block[s, 3 * rows :].astype(F32), rows, stride0, ex)
                for s in range(half)
            ],
            axis=0,
        )
        extra = jnp.where((q_lanes >= ex) & (q_lanes < 2 * ex), extra, bias_one)
        top = jnp.concatenate([jnp.where(first_head, qa, 0.0), bias_one], axis=1)
        low = jnp.concatenate([jnp.where(first_head, 0.0, qa), extra], axis=1)
        return jnp.concatenate([top, low], axis=0).astype(BF16)

    bases = [(1 - near) * half, near * half]
    queries = [queries_of(base) for base in bases]

    def attend(i, keys, values, first):
        scores = dot_t(queries[i], keys)
        top = jnp.max(scores, axis=1, keepdims=True)
        if not first:
            before = top_s[i][:, 0:1]
            top = jnp.maximum(top, before)
        prob = jnp.exp2(scores - top).astype(BF16)
        mixed = dot(prob, values)
        if not first:
            mixed = o_s[i] * jnp.exp2(before - top) + mixed
        return top, mixed

    def keep(i, state):
        top_s[i] = jnp.broadcast_to(state[0], top_s.shape[1:])
        o_s[i] = state[1]

    for g in range(groups):
        keys, values = keys_of(got0, g, 1, fold0, stride0, 0)
        for i in range(2):
            keep(i, attend(i, keys, values, g == 0))

    drain(got1.at[pl.ds(0, slots - 1)], rrecv)
    for g in range(groups - 1):
        keys, values = keys_of(got1, g, 0, fold1, stride1, ex)
        for i in range(2):
            keep(i, attend(i, keys, values, False))

    keys, values = keys_of(got1, groups - 1, 0, fold1, stride1, ex)
    fold_zero = jnp.zeros((fold2, LANE), F32)
    for i in range(2):
        _, mixed = attend(i, keys, values, False)
        share = 1.0 / mixed[:, LANE + 3 * ex : LANE + 3 * ex + 1]
        mixed = mixed * share
        main = jnp.where(first_head, mixed[:cells, :LANE], mixed[cells:, :LANE])
        extra = mixed[cells:, LANE:]
        for s in range(half):
            span_s = slice(s * rows, (s + 1) * rows)
            slot = bases[i] + s
            att[slot, :rows, :] = main[span_s].astype(BF16)
            att[slot, rows:, :] = fold(
                [extra[span_s]], fold_zero, fold2, ex, ex, 2 * ex
            ).astype(BF16)
        for s in range(half):
            slot = bases[i] + s

            @pl.when(slot != pair)
            def _():
                remote(
                    att.at[slot], back.at[pair], asend, arecv, me - pair + slot
                ).start()

    back[pair] = att[pair]
    ow_load.wait()
    drain(gates.at[pl.ds(0, n - 1)], grecv)
    gate_rows = jnp.sum(gates[...].astype(F32), axis=0)
    gate = jnp.concatenate([gate_rows[0:1], gate_rows[1:2, 2 * span - width :]], axis=1)
    valid = (lax.broadcasted_iota(jnp.int32, (rows, 1), 0) < counts[me]).astype(F32)

    drain(mods.at[pl.ds(0, n - 1)], msend)
    drain(gates.at[pl.ds(0, n - 1)], gsend)
    mirror_copy.wait_send()
    drain(got0.at[pl.ds(0, slots - 1)], psend)
    drain(got1.at[pl.ds(0, slots - 1)], rsend)
    drain(back.at[pl.ds(0, PAIRS - 1)], arecv)

    rest = jnp.zeros((rows, LANE), F32)
    for p in range(PAIRS):
        piece = unfold(back[p, rows:, :].astype(F32), rows, ex, p * ex)
        rest = jnp.where((lane_ids >= p * ex) & (lane_ids < (p + 1) * ex), piece, rest)
    chunks = []
    for c in range(PAIRS + 1):
        here = back[c, :rows, :].astype(F32) if c < PAIRS else rest
        if c:
            here = jnp.where(lane_ids < c * ex, rest, here)
            here = jnp.where(lane_ids < (c - 1) * ex, back[c - 1, :rows, :].astype(F32), here)
        chunks.append(here)
    attended = jnp.concatenate(chunks, axis=1).astype(BF16)
    projected = dot(attended, ow[...])
    out[...] = (xin_s[...] + gate * projected * valid).astype(BF16)
    drain(back.at[pl.ds(0, PAIRS - 1)], asend)


def tables(width, freq):
    quarter, half = width // 4, freq // 2
    omega = np.power(10000.0, -np.arange(quarter) / quarter)
    turn = math.pi / 2
    pos_tab = np.stack([np.tile(omega, 4), np.repeat([0.0, turn, 0.0, turn], quarter)])
    wave = np.exp(-math.log(10000.0) * np.arange(half) / half)
    time_tab = np.stack([np.tile(wave, 2), np.repeat([turn, 0.0], half)])
    return pos_tab.astype(np.float32), time_tab.astype(np.float32)


def per_device(
    tokens, positions, counts, timestep, time_in, time_out, ada_weight, qkv_weight, out_weight
):
    n = lax.axis_size("patch")
    rows, width = tokens.shape
    head = width // HEADS
    ex = 2 * head - LANE
    assert 0 < ex and PAIRS * ex <= LANE and n % HEADS == 0
    size0 = 3 * rows + fold_rows(rows, 3 * ex + 2)
    size1 = 2 * rows + fold_rows(rows, 2 * ex + 2)
    size2 = rows + fold_rows(rows, ex)
    slots = n // 2
    queries = PAIRS * rows
    pos_tab, time_tab = tables(width, time_in.shape[0])
    hbm = pl.BlockSpec(memory_space=pl.ANY)
    vmem = pl.BlockSpec(memory_space=pltpu.VMEM)
    dma = pltpu.SemaphoreType.DMA
    return pl.pallas_call(
        functools.partial(block_kernel, n, rows, width, head),
        out_shape=pltpu.VMEM((rows, width), BF16),
        in_specs=[hbm] * 11,
        out_specs=vmem,
        scratch_shapes=[
            pltpu.SMEM(counts.shape, jnp.int32),
            pltpu.SMEM(timestep.shape, jnp.int32),
            pltpu.VMEM(positions.shape, jnp.int32),
            pltpu.VMEM(pos_tab.shape, F32),
            pltpu.VMEM(time_tab.shape, F32),
            pltpu.VMEM(tokens.shape, BF16),
            pltpu.VMEM(time_in.shape, BF16),
            pltpu.VMEM(time_out.shape[::-1], BF16),
            pltpu.VMEM(ada_weight.shape, BF16),
            pltpu.VMEM(qkv_weight.shape, BF16),
            pltpu.VMEM(out_weight.shape, BF16),
            pltpu.VMEM((n, 2, width), BF16),
            pltpu.VMEM((n, 2, -(-width // 256) * 128), BF16),
            pltpu.VMEM((rows, width), F32),
            pltpu.VMEM((rows, width), F32),
            pltpu.VMEM((rows, width), BF16),
            pltpu.VMEM((rows, width), BF16),
            pltpu.VMEM((PAIRS, size0, LANE), BF16),
            pltpu.VMEM((PAIRS, size1, LANE), BF16),
            pltpu.VMEM((slots, size0, LANE), BF16),
            pltpu.VMEM((slots, size1, LANE), BF16),
            pltpu.VMEM((2, queries, 2 * LANE), F32),
            pltpu.VMEM((2, queries, LANE), F32),
            pltpu.VMEM((PAIRS, size2, LANE), BF16),
            pltpu.VMEM((PAIRS, size2, LANE), BF16),
            dma((5,)),
            dma((5,)),
        ]
        + [dma((1,))] * 13,
        compiler_params=pltpu.CompilerParams(
            collective_id=0, has_side_effects=True, vmem_limit_bytes=60 * 2**20
        ),
    )(
        counts, timestep, positions, pos_tab, time_tab,
        tokens, time_in, time_out.T, ada_weight, qkv_weight, out_weight,
    )


def solution(mesh):
    placed = (
        P(("req", "patch"), None),
        P(None, ("req", "patch")),
        P("req"),
        P("req"),
        P(),
        P(None, "patch"),
        P("patch", None),
        P(),
        P(),
    )
    return jax.shard_map(
        per_device, mesh=mesh, in_specs=placed, out_specs=P(("req", "patch"), None), check_vma=False
    )
```

```python
import functools
import math

import jax
import jax.numpy as jnp
import numpy as np
from jax import lax
from jax.experimental import pallas as pl
from jax.experimental.pallas import tpu as pltpu
from jax.sharding import PartitionSpec as P

HEADS = 16
PAIRS = HEADS // 2
LANE = 128
NEG = -1e30
F32 = jnp.float32
BF16 = jnp.bfloat16
MESH = pl.DeviceIdType.MESH
PI_PARTS = (3.140625, 0.000967502593994140625, 1.509957990978376432e-07)


def silu(v):
    return v / (1.0 + jnp.exp(-v))


def sine(x):
    turns = jnp.floor(x * (1.0 / math.pi) + 0.5)
    r = x - turns * PI_PARTS[0]
    r = r - turns * PI_PARTS[1]
    r = r - turns * PI_PARTS[2]
    s = r * r
    poly = -2.3889859e-08 * s + 2.7525562e-06
    poly = poly * s - 0.00019840874
    poly = poly * s + 0.0083333310
    poly = poly * s - 0.16666667
    value = r + r * (s * poly)
    odd = turns - 2.0 * jnp.floor(turns * 0.5)
    return value * (1.0 - 2.0 * odd)


def dot(a, b):
    return jnp.dot(a, b, preferred_element_type=F32)


def dot_t(a, b):
    return lax.dot_general(a, b, (((1,), (1,)), ((), ())), preferred_element_type=F32)


def one_row_dot(row, matrix):
    wide = jnp.broadcast_to(row, (16, row.shape[1])).astype(BF16)
    return dot(wide, matrix)[0:1]


def fold_rows(rows, stride):
    group = 8
    while rows % group or rows // group * stride > LANE:
        group += 8
    return group


def turned(x, shift):
    if isinstance(shift, int):
        shift %= LANE
        return pltpu.roll(x, shift, axis=1) if shift else x
    return pltpu.roll(x, lax.rem(shift + LANE, LANE), axis=1)


def flip(index, bit):
    return index + bit * (1 - 2 * lax.rem(index // bit, 2))


def fold(blocks, base, group, stride, ex, at):
    lanes = lax.broadcasted_iota(jnp.int32, (group, LANE), 1)
    packed = base
    for r in range(blocks[0].shape[0] // group):
        for j, block in enumerate(blocks):
            low = r * stride + j * ex
            piece = turned(block[r * group : (r + 1) * group], low - at)
            packed = jnp.where((lanes >= low) & (lanes < low + ex), piece, packed)
    return packed


def unfold(packed, rows, stride, to):
    group = packed.shape[0]
    return jnp.concatenate(
        [turned(packed, to - r * stride) for r in range(rows // group)], axis=0
    )


def block_kernel(
    n, rows, width, head,
    counts_h, tstep_h, pos_h, pos_tab_h, time_tab_h,
    tok_h, tin_h, tout_h, ada_h, qkv_h, ow_h,
    out,
    counts, tstep, pos, pos_tab, time_tab, tok, tin, tout, ada, near_w, far_w, kv_w, ow,
    mods, gates, msum, mgot, gsum, ggot, xin_s, norm_s, nsend, ngot, xgot, zgot, sendd, sendp, send1, send2,
    got0, got1, got2, o_s, top_s, att, back,
    lsem, ssem, wsem, msend, mrecv, gsend, grecv, nsem, nrecv, dsend, drecv, psend, precv,
    rsend, rrecv, tsend, trecv, asend, arecv, hsend, hrecv, fsend, frecv,
):
    me = lax.axis_index("patch")
    pair = lax.rem(me, PAIRS)
    side = lax.rem(me // PAIRS, 2)
    group = me // HEADS
    groups = n // HEADS
    mirror = me + PAIRS * (1 - 2 * side)
    ex = 2 * head - LANE
    stride0, stride1 = 3 * ex + 2, 2 * ex + 2
    fold0, fold1, fold2 = fold_rows(rows, stride0), fold_rows(rows, stride1), fold_rows(rows, ex)
    scale_q = math.log2(math.e) / math.sqrt(head)

    barrier = pltpu.get_barrier_semaphore()

    def drain(ref, sem):
        pltpu.make_async_copy(ref, ref, sem.at[0]).wait()

    def remote(src, dst, send, recv, to):
        return pltpu.make_async_remote_copy(
            src_ref=src, dst_ref=dst, send_sem=send.at[0], recv_sem=recv.at[0],
            device_id={"patch": to}, device_id_type=MESH,
        )

    @pl.loop(1, n)
    def _(step):
        pl.semaphore_signal(
            barrier, inc=1, device_id={"patch": lax.rem(me + step, n)}, device_id_type=MESH
        )

    loads = [
        pltpu.make_async_copy(src, dst, lsem.at[i])
        for i, (src, dst) in enumerate(
            [(tin_h, tin), (tout_h, tout), (ada_h, ada), (tok_h, tok)]
        )
    ]
    chip = pair // 2
    far_chip = flip(flip(pair, 2), 4) // 2
    reach = near_w.shape[1] // 3

    def window(i, owner):
        return pl.ds(pl.multiple_of(i * width + 2 * LANE * owner, LANE), reach)

    qkv_loads = [
        pltpu.make_async_copy(
            qkv_h.at[:, window(i, owner)], dst.at[:, pl.ds(i * reach, reach)], wsem.at[k]
        )
        for k, (owner, dst) in ((1, (far_chip, far_w)), (2, (chip, near_w)))
        for i in range(3)
    ]
    qkv_loads.insert(3, pltpu.make_async_copy(qkv_h.at[:, pl.ds(width, 2 * width)], kv_w, wsem.at[3]))
    small = [
        pltpu.make_async_copy(src, dst, ssem.at[i])
        for i, (src, dst) in enumerate(
            [(tstep_h, tstep), (time_tab_h, time_tab), (counts_h, counts),
             (pos_h, pos), (pos_tab_h, pos_tab)]
        )
    ]
    for load in small[:2] + loads[:4] + small[2:]:
        load.start()
    for load in small[:2]:
        load.wait()

    angles = tstep[0].astype(F32) * time_tab[0:1, :] + time_tab[1:2, :]
    features = sine(angles).astype(BF16)
    loads[0].wait()
    hidden = silu(one_row_dot(features, tin[...])).astype(BF16)
    loads[1].wait()
    wide = jnp.broadcast_to(hidden, (16, width))
    cond = dot_t(wide, tout[...])
    activated = silu(cond[0:1]).astype(BF16)
    loads[2].wait()
    partial = one_row_dot(activated, ada[...])
    mods[me // 2] = jnp.concatenate(
        [partial[:, :width], partial[:, width : 2 * width]], axis=0
    ).astype(BF16)
    span = gates.shape[2]
    gates[me // 2] = jnp.concatenate(
        [partial[:, 2 * width : 2 * width + span], partial[:, 3 * width - span :]], axis=0
    ).astype(BF16)
    for load in qkv_loads:
        load.start()
    ow_load = pltpu.make_async_copy(ow_h, ow, wsem.at[0])
    ow_load.start()

    pl.semaphore_wait(barrier, n - 1)

    half_n = n // 2

    @pl.loop(1, half_n)
    def _(step):
        row = me // 2
        remote(mods.at[row], mods.at[row], msend, mrecv, lax.rem(me + 2 * step, n)).start()

    ids = lax.broadcasted_iota(jnp.int32, (rows, rows), 0)
    eye = ids == lax.broadcasted_iota(jnp.int32, (rows, rows), 1)
    for load in small[2:]:
        load.wait()
    posf = pos[...].astype(F32)
    row_col = jnp.sum(jnp.where(eye, posf[0:1, :], 0.0), axis=1, keepdims=True)
    col_col = jnp.sum(jnp.where(eye, posf[1:2, :], 0.0), axis=1, keepdims=True)
    wide_lanes = lax.broadcasted_iota(jnp.int32, (1, width), 1)
    place = jnp.where(wide_lanes < width // 2, row_col, col_col)
    embed = sine(place * pos_tab[0:1, :] + pos_tab[1:2, :])
    loads[3].wait()
    x_in = tok[...].astype(F32) + embed
    xin_s[...] = x_in
    centered = x_in - jnp.mean(x_in, axis=1, keepdims=True)
    variance = jnp.mean(centered * centered, axis=1, keepdims=True)
    norm = centered * lax.rsqrt(variance + 1e-6)
    norm_s[...] = norm
    nsend[...] = norm.astype(BF16)
    norm_copies = [
        pltpu.make_async_remote_copy(
            src_ref=nsend, dst_ref=dst, send_sem=nsem.at[i], recv_sem=nrecv.at[i],
            device_id={"patch": to}, device_id_type=MESH,
        )
        for i, (dst, to) in enumerate([(ngot, mirror), (zgot, flip(me, 4)), (xgot, flip(me, 2))])
    ]
    for copy in norm_copies:
        copy.start()

    drain(mods.at[pl.ds(0, half_n - 1)], mrecv)
    partner = flip(me, 1)
    msum[...] = jnp.sum(mods[...].astype(F32), axis=0)
    sum_copy = remote(msum, mgot, hsend, hrecv, partner)
    sum_copy.start()
    sum_copy.wait_recv()
    modulation = msum[...] + mgot[...]
    shift = modulation[0:1]
    gain = 1.0 + modulation[1:2]
    modulated = (norm_s[...] * gain + shift).astype(BF16)

    lane_ids = lax.broadcasted_iota(jnp.int32, (rows, LANE), 1)

    def base_of(owner, fold_group, stride, blocks):
        lanes = lax.broadcasted_iota(jnp.int32, (fold_group, LANE), 1)
        slot = lax.broadcasted_iota(jnp.int32, (fold_group, LANE), 0)
        base = jnp.zeros((fold_group, LANE), F32)
        for r in range(rows // fold_group):
            low = r * stride + blocks * ex
            base = jnp.where(lanes == low, 1.0, base)
            bias = jnp.where(slot + r * fold_group < counts[owner], 0.0, NEG)
            base = jnp.where(lanes == low + 1, bias, base)
        return base

    def pack(parts, p, low, base, fold_group, stride, write):
        cut = p * ex
        nexts = []
        for j, part in enumerate(parts):
            here = part[:, low : low + LANE]
            after = part[:, low + LANE : low + 2 * LANE]
            nexts.append(after)
            mixed = jnp.where(lane_ids < cut, after, here)
            write(slice(j * rows, (j + 1) * rows), mixed.astype(BF16))
        packed = fold(nexts, base, fold_group, stride, ex, cut)
        write(slice(len(parts) * rows, None), packed.astype(BF16))

    def into(ref, index):
        def write(part, value):
            ref[index, part, :] = value

        return write

    def pair_parts(x, weights):
        product = dot(x, weights[...])
        parts = [product[:, i * reach : (i + 1) * reach] for i in range(3)]
        return [parts[0] * scale_q] + parts[1:]

    my_slot = group * PAIRS + pair
    slots = groups * PAIRS
    block_of = me - pair
    pltpu.make_async_copy(far_w, far_w, wsem.at[1]).wait()
    base0 = base_of(me, fold0, stride0, 3)
    parts = pair_parts(modulated, far_w)
    for q in range(2):
        pack(parts, 2 * far_chip + q, q * LANE, base0, fold0, stride0, into(sendd, q))
    for q in range(2):
        remote(sendd.at[q], got0.at[pair], dsend, drecv, block_of + 2 * far_chip + q).start()

    pltpu.make_async_copy(kv_w, kv_w, wsem.at[3]).wait()

    def kv_pack(x, owner, buffer):
        base = base_of(owner, fold1, stride1, 2)
        parts = [dot(x, kv_w[:, i * width : (i + 1) * width]) for i in range(2)]
        for p in range(PAIRS):
            pack(parts, p, p * LANE, base, fold1, stride1, into(buffer, p))

    def spread(buffer, got, send, recv, g):
        for j in range(1 if g is None else 0, PAIRS):
            turn = lax.rem(pair + j, PAIRS)
            to = (group if g is None else g) * HEADS + side * PAIRS + turn
            remote(buffer.at[turn], got.at[my_slot], send, recv, to).start()

    if groups > 1:
        kv_pack(modulated, me, send2)

        @pl.loop(1, groups)
        def _(g):
            spread(send2, got2, tsend, trecv, lax.rem(group + g, groups))

    norm_copies[0].wait_recv()
    kv_pack((ngot[...].astype(F32) * gain + shift).astype(BF16), mirror, send1)
    spread(send1, got1, rsend, rrecv, None)
    if groups > 1:

        @pl.loop(1, groups)
        def _(g):
            spread(send1, got1, rsend, rrecv, lax.rem(group + g, groups))

    got1[my_slot] = send1[pair]

    @pl.loop(1, half_n)
    def _(step):
        row = me // 2
        remote(gates.at[row], gates.at[row], gsend, grecv, lax.rem(me + 2 * step, n)).start()

    pltpu.make_async_copy(near_w, near_w, wsem.at[2]).wait()
    norm_copies[1].wait_recv()
    norm_copies[2].wait_recv()
    others = [(ref[...].astype(F32) * gain + shift).astype(BF16) for ref in (xgot, zgot)]
    parts = pair_parts(jnp.concatenate([modulated] + others, axis=0), near_w)
    owners = [pair, flip(pair, 2), flip(pair, 4)]
    bases = [base0] + [base_of(block_of + owner, fold0, stride0, 3) for owner in owners[1:]]
    mine = lax.rem(pair, 2)
    for b in range(3):
        own = [part[b * rows : (b + 1) * rows] for part in parts]
        for q in range(2):
            pack(own, 2 * chip + q, q * LANE, bases[b], fold0, stride0, into(sendp, 2 * b + q))
    for b in range(3):
        remote(sendp.at[2 * b + 1 - mine], got0.at[owners[b]], psend, precv, partner).start()
    for b in range(3):
        got0[owners[b]] = sendp[2 * b + mine]

    drain(got0.at[pl.ds(0, 3)], precv)
    drain(got0.at[pl.ds(0, 2)], drecv)

    def keys_of(got, g, first, fold_group, stride, to):
        block = got[pl.ds(g * PAIRS, PAIRS)]
        cells = PAIRS * rows
        k = block[:, first * rows : (first + 1) * rows].reshape(cells, LANE)
        v = block[:, (first + 1) * rows : (first + 2) * rows].reshape(cells, LANE)
        extra = jnp.concatenate(
            [unfold(block[s, (first + 2) * rows :].astype(F32), rows, stride, to) for s in range(PAIRS)],
            axis=0,
        ).astype(BF16)
        return jnp.concatenate([k, extra], axis=1), jnp.concatenate([v, extra], axis=1)

    half = PAIRS // 2
    cells = half * rows
    near = pair // half
    q_lanes = lax.broadcasted_iota(jnp.int32, (cells, LANE), 1)
    column = lax.rem(q_lanes + (LANE - ex * pair), LANE)
    first_head = column < head
    bias_one = jnp.where(q_lanes == 3 * ex + 1, 1.0, 0.0)

    def queries_of(base):
        block = got0[pl.ds(base, half)]
        qa = block[:, :rows].reshape(cells, LANE).astype(F32)
        extra = jnp.concatenate(
            [
                unfold(block[s, 3 * rows :].astype(F32), rows, stride0, ex)
                for s in range(half)
            ],
            axis=0,
        )
        extra = jnp.where((q_lanes >= ex) & (q_lanes < 2 * ex), extra, bias_one)
        top = jnp.concatenate([jnp.where(first_head, qa, 0.0), bias_one], axis=1)
        low = jnp.concatenate([jnp.where(first_head, 0.0, qa), extra], axis=1)
        return jnp.concatenate([top, low], axis=0).astype(BF16)

    starts = [(1 - near) * half, near * half]
    queries = [queries_of(base) for base in starts]

    def attend(i, keys, values, first):
        scores = dot_t(queries[i], keys)
        top = jnp.max(scores, axis=1, keepdims=True)
        if not first:
            before = top_s[i][:, 0:1]
            top = jnp.maximum(top, before)
        prob = jnp.exp2(scores - top).astype(BF16)
        mixed = dot(prob, values)
        if not first:
            mixed = o_s[i] * jnp.exp2(before - top) + mixed
        return top, mixed

    def keep(i, state):
        top_s[i] = jnp.broadcast_to(state[0], top_s.shape[1:])
        o_s[i] = state[1]

    keys, values = keys_of(got0, 0, 1, fold0, stride0, 0)
    for i in range(2):
        keep(i, attend(i, keys, values, True))

    if groups > 1:
        drain(got2.at[pl.ds(0, slots - PAIRS)], trecv)
    drain(got1.at[pl.ds(0, slots - 1)], rrecv)
    for g in range(1, groups):
        other = lax.rem(group + g, groups)
        for got in (got1, got2):
            keys, values = keys_of(got, other, 0, fold1, stride1, ex)
            for i in range(2):
                keep(i, attend(i, keys, values, False))

    keys, values = keys_of(got1, group, 0, fold1, stride1, ex)
    fold_zero = jnp.zeros((fold2, LANE), F32)
    for i in range(2):
        _, mixed = attend(i, keys, values, False)
        share = 1.0 / mixed[:, LANE + 3 * ex : LANE + 3 * ex + 1]
        mixed = mixed * share
        main = jnp.where(first_head, mixed[:cells, :LANE], mixed[cells:, :LANE])
        extra = mixed[cells:, LANE:]
        for s in range(half):
            span_s = slice(s * rows, (s + 1) * rows)
            slot = starts[i] + s
            att[slot, :rows, :] = main[span_s].astype(BF16)
            att[slot, rows:, :] = fold(
                [extra[span_s]], fold_zero, fold2, ex, ex, 2 * ex
            ).astype(BF16)
        for s in range(i, half):
            slot = starts[i] + lax.rem(pair + s, half)
            remote(att.at[slot], back.at[pair], asend, arecv, me - pair + slot).start()

    drain(gates.at[pl.ds(0, half_n - 1)], grecv)
    gsum[...] = jnp.sum(gates[...].astype(F32), axis=0)
    gate_copy = remote(gsum, ggot, fsend, frecv, partner)
    gate_copy.start()
    back[pair] = att[pair]
    ow_load.wait()
    valid = (lax.broadcasted_iota(jnp.int32, (rows, 1), 0) < counts[me]).astype(F32)

    drain(mods.at[pl.ds(0, half_n - 1)], msend)
    drain(gates.at[pl.ds(0, half_n - 1)], gsend)
    sum_copy.wait_send()
    for copy in norm_copies:
        copy.wait_send()
    drain(got0.at[pl.ds(0, 2)], dsend)
    drain(got0.at[pl.ds(0, 3)], psend)
    if groups > 1:
        drain(got2.at[pl.ds(0, slots - PAIRS)], tsend)
    drain(got1.at[pl.ds(0, slots - 1)], rsend)
    drain(back.at[pl.ds(0, PAIRS - 1)], arecv)

    gate_copy.wait()
    gate_rows = gsum[...] + ggot[...]
    gate = jnp.concatenate([gate_rows[0:1], gate_rows[1:2, 2 * span - width :]], axis=1)
    rest = jnp.zeros((rows, LANE), F32)
    for p in range(PAIRS):
        piece = unfold(back[p, rows:, :].astype(F32), rows, ex, p * ex)
        rest = jnp.where((lane_ids >= p * ex) & (lane_ids < (p + 1) * ex), piece, rest)
    chunks = []
    for c in range(PAIRS + 1):
        here = back[c, :rows, :].astype(F32) if c < PAIRS else rest
        if c:
            here = jnp.where(lane_ids < c * ex, rest, here)
            here = jnp.where(lane_ids < (c - 1) * ex, back[c - 1, :rows, :].astype(F32), here)
        chunks.append(here)
    attended = jnp.concatenate(chunks, axis=1).astype(BF16)
    projected = dot(attended, ow[...])
    out[...] = (xin_s[...] + gate * projected * valid).astype(BF16)
    drain(back.at[pl.ds(0, PAIRS - 1)], asend)


def tables(width, freq):
    quarter, half = width // 4, freq // 2
    omega = np.power(10000.0, -np.arange(quarter) / quarter)
    turn = math.pi / 2
    pos_tab = np.stack([np.tile(omega, 4), np.repeat([0.0, turn, 0.0, turn], quarter)])
    wave = np.exp(-math.log(10000.0) * np.arange(half) / half)
    time_tab = np.stack([np.tile(wave, 2), np.repeat([turn, 0.0], half)])
    return pos_tab.astype(np.float32), time_tab.astype(np.float32)


def per_device(
    tokens, positions, counts, timestep, time_in, time_out, ada_weight, qkv_weight, out_weight
):
    n = lax.axis_size("patch")
    rows, width = tokens.shape
    head = width // HEADS
    ex = 2 * head - LANE
    assert 0 < ex and PAIRS * ex <= LANE and n % HEADS == 0
    size0 = 3 * rows + fold_rows(rows, 3 * ex + 2)
    size1 = 2 * rows + fold_rows(rows, 2 * ex + 2)
    size2 = rows + fold_rows(rows, ex)
    slots = n // 2
    queries = PAIRS * rows
    span = -(-width // 256) * LANE
    pos_tab, time_tab = tables(width, time_in.shape[0])
    hbm = pl.BlockSpec(memory_space=pl.ANY)
    vmem = pl.BlockSpec(memory_space=pltpu.VMEM)
    dma = pltpu.SemaphoreType.DMA
    return pl.pallas_call(
        functools.partial(block_kernel, n, rows, width, head),
        out_shape=pltpu.VMEM((rows, width), BF16),
        in_specs=[hbm] * 11,
        out_specs=vmem,
        scratch_shapes=[
            pltpu.SMEM(counts.shape, jnp.int32),
            pltpu.SMEM(timestep.shape, jnp.int32),
            pltpu.VMEM(positions.shape, jnp.int32),
            pltpu.VMEM(pos_tab.shape, F32),
            pltpu.VMEM(time_tab.shape, F32),
            pltpu.VMEM(tokens.shape, BF16),
            pltpu.VMEM(time_in.shape, BF16),
            pltpu.VMEM(time_out.shape[::-1], BF16),
            pltpu.VMEM(ada_weight.shape, BF16),
            pltpu.VMEM((width, 9 * LANE), BF16),
            pltpu.VMEM((width, 9 * LANE), BF16),
            pltpu.VMEM((width, 2 * width), BF16),
            pltpu.VMEM(out_weight.shape, BF16),
            pltpu.VMEM((n // 2, 2, width), BF16),
            pltpu.VMEM((n // 2, 2, span), BF16),
            pltpu.VMEM((2, width), F32),
            pltpu.VMEM((2, width), F32),
            pltpu.VMEM((2, span), F32),
            pltpu.VMEM((2, span), F32),
            pltpu.VMEM((rows, width), F32),
            pltpu.VMEM((rows, width), F32),
            pltpu.VMEM((rows, width), BF16),
            pltpu.VMEM((rows, width), BF16),
            pltpu.VMEM((rows, width), BF16),
            pltpu.VMEM((rows, width), BF16),
            pltpu.VMEM((2, size0, LANE), BF16),
            pltpu.VMEM((6, size0, LANE), BF16),
            pltpu.VMEM((PAIRS, size1, LANE), BF16),
            pltpu.VMEM((PAIRS, size1, LANE), BF16),
            pltpu.VMEM((PAIRS, size0, LANE), BF16),
            pltpu.VMEM((slots, size1, LANE), BF16),
            pltpu.VMEM((slots, size1, LANE), BF16),
            pltpu.VMEM((2, queries, 2 * LANE), F32),
            pltpu.VMEM((2, queries, LANE), F32),
            pltpu.VMEM((PAIRS, size2, LANE), BF16),
            pltpu.VMEM((PAIRS, size2, LANE), BF16),
            dma((5,)),
            dma((5,)),
        ]
        + [dma((4,))] + [dma((1,))] * 4 + [dma((3,))] * 2 + [dma((1,))] * 14,
        compiler_params=pltpu.CompilerParams(
            collective_id=0, has_side_effects=True, vmem_limit_bytes=60 * 2**20
        ),
    )(
        counts, timestep, positions, pos_tab, time_tab,
        tokens, time_in, time_out.T, ada_weight, qkv_weight, out_weight,
    )


def solution(mesh):
    placed = (
        P(("req", "patch"), None),
        P(None, ("req", "patch")),
        P("req"),
        P("req"),
        P(),
        P(None, "patch"),
        P("patch", None),
        P(),
        P(),
    )
    return jax.shard_map(
        per_device, mesh=mesh, in_specs=placed, out_specs=P(("req", "patch"), None), check_vma=False
    )
```

```python
import functools
import math

import jax
import jax.numpy as jnp
import numpy as np
from jax import lax
from jax.experimental import pallas as pl
from jax.experimental.pallas import tpu as pltpu
from jax.sharding import PartitionSpec as P

HEADS = 16
PAIRS = HEADS // 2
LANE = 128
NEG = -1e30
F32 = jnp.float32
BF16 = jnp.bfloat16
MESH = pl.DeviceIdType.MESH
PI_PARTS = (3.140625, 0.000967502593994140625, 1.509957990978376432e-07)


def silu(v):
    return v / (1.0 + jnp.exp(-v))


def sine(x):
    turns = jnp.floor(x * (1.0 / math.pi) + 0.5)
    r = x - turns * PI_PARTS[0]
    r = r - turns * PI_PARTS[1]
    r = r - turns * PI_PARTS[2]
    s = r * r
    poly = -2.3889859e-08 * s + 2.7525562e-06
    poly = poly * s - 0.00019840874
    poly = poly * s + 0.0083333310
    poly = poly * s - 0.16666667
    value = r + r * (s * poly)
    odd = turns - 2.0 * jnp.floor(turns * 0.5)
    return value * (1.0 - 2.0 * odd)


def dot(a, b):
    return jnp.dot(a, b, preferred_element_type=F32)


def dot_t(a, b):
    return lax.dot_general(a, b, (((1,), (1,)), ((), ())), preferred_element_type=F32)


def one_row_dot(row, matrix):
    wide = jnp.broadcast_to(row, (16, row.shape[1])).astype(BF16)
    return dot(wide, matrix)[0:1]


def fold_rows(rows, stride):
    group = 8
    while rows % group or rows // group * stride > LANE:
        group += 8
    return group


def turned(x, shift):
    if isinstance(shift, int):
        shift %= LANE
        return pltpu.roll(x, shift, axis=1) if shift else x
    return pltpu.roll(x, lax.rem(shift + LANE, LANE), axis=1)


def flip(index, bit):
    return index + bit * (1 - 2 * lax.rem(index // bit, 2))


def fold(blocks, base, group, stride, ex, at):
    lanes = lax.broadcasted_iota(jnp.int32, (group, LANE), 1)
    packed = base
    for r in range(blocks[0].shape[0] // group):
        for j, block in enumerate(blocks):
            low = r * stride + j * ex
            piece = turned(block[r * group : (r + 1) * group], low - at)
            packed = jnp.where((lanes >= low) & (lanes < low + ex), piece, packed)
    return packed


def unfold(packed, rows, stride, to):
    group = packed.shape[0]
    return jnp.concatenate(
        [turned(packed, to - r * stride) for r in range(rows // group)], axis=0
    )


def block_kernel(
    n, rows, width, head,
    counts_h, tstep_h, pos_h, pos_tab_h, time_tab_h,
    tok_h, tin_h, tout_h, ada_h, qkv_h, ow_h,
    out,
    counts, tstep, pos, pos_tab, time_tab, tok, tin, tout, ada, near_w, far_w, kv_w, ow,
    mods, gates, msum, mgot, gsum, ggot, xin_s, norm_s, nsend, ngot, xgot, zgot, sendd, sendp, send1, send2,
    got0, got1, got2, o_s, top_s, total_s, att, back,
    lsem, ssem, wsem, msend, mrecv, gsend, grecv, nsem, nrecv, dsend, drecv, psend, precv,
    rsend, rrecv, tsend, trecv, asend, arecv, hsend, hrecv, fsend, frecv,
):
    me = lax.axis_index("patch")
    pair = lax.rem(me, PAIRS)
    side = lax.rem(me // PAIRS, 2)
    group = me // HEADS
    groups = n // HEADS
    mirror = flip(flip(me, PAIRS), PAIRS // 2)
    ex = 2 * head - LANE
    stride0, stride1 = 3 * ex + 2, 2 * ex + 2
    fold0, fold1, fold2 = fold_rows(rows, stride0), fold_rows(rows, stride1), fold_rows(rows, ex)
    scale_q = math.log2(math.e) / math.sqrt(head)

    barrier = pltpu.get_barrier_semaphore()

    def drain(ref, sem):
        pltpu.make_async_copy(ref, ref, sem.at[0]).wait()

    def remote(src, dst, send, recv, to):
        return pltpu.make_async_remote_copy(
            src_ref=src, dst_ref=dst, send_sem=send.at[0], recv_sem=recv.at[0],
            device_id={"patch": to}, device_id_type=MESH,
        )

    @pl.loop(1, n)
    def _(step):
        pl.semaphore_signal(
            barrier, inc=1, device_id={"patch": lax.rem(me + step, n)}, device_id_type=MESH
        )

    loads = [
        pltpu.make_async_copy(src, dst, lsem.at[i])
        for i, (src, dst) in enumerate(
            [(tin_h, tin), (tout_h, tout), (ada_h, ada), (tok_h, tok)]
        )
    ]
    chip = pair // 2
    far_chip = flip(flip(pair, 2), 4) // 2
    reach = near_w.shape[1] // 3

    def window(i, owner):
        return pl.ds(pl.multiple_of(i * width + 2 * LANE * owner, LANE), reach)

    qkv_loads = [
        pltpu.make_async_copy(
            qkv_h.at[:, window(i, owner)], dst.at[:, pl.ds(i * reach, reach)], wsem.at[k]
        )
        for k, (owner, dst) in ((1, (far_chip, far_w)), (2, (chip, near_w)))
        for i in range(3)
    ]
    qkv_loads.insert(3, pltpu.make_async_copy(qkv_h.at[:, pl.ds(width, 2 * width)], kv_w, wsem.at[3]))
    small = [
        pltpu.make_async_copy(src, dst, ssem.at[i])
        for i, (src, dst) in enumerate(
            [(tstep_h, tstep), (time_tab_h, time_tab), (counts_h, counts),
             (pos_h, pos), (pos_tab_h, pos_tab)]
        )
    ]
    for load in small[2:] + loads[3:] + small[:2] + loads[:3]:
        load.start()

    ids = lax.broadcasted_iota(jnp.int32, (rows, rows), 0)
    eye = ids == lax.broadcasted_iota(jnp.int32, (rows, rows), 1)
    for load in small[2:]:
        load.wait()
    posf = pos[...].astype(F32)
    row_col = jnp.sum(jnp.where(eye, posf[0:1, :], 0.0), axis=1, keepdims=True)
    col_col = jnp.sum(jnp.where(eye, posf[1:2, :], 0.0), axis=1, keepdims=True)
    wide_lanes = lax.broadcasted_iota(jnp.int32, (1, width), 1)
    place = jnp.where(wide_lanes < width // 2, row_col, col_col)
    embed = sine(place * pos_tab[0:1, :] + pos_tab[1:2, :])
    loads[3].wait()
    x_in = tok[...].astype(F32) + embed
    xin_s[...] = x_in
    centered = x_in - jnp.mean(x_in, axis=1, keepdims=True)
    variance = jnp.mean(centered * centered, axis=1, keepdims=True)
    norm = centered * lax.rsqrt(variance + 1e-6)
    norm_s[...] = norm
    nsend[...] = norm.astype(BF16)
    for load in small[:2]:
        load.wait()
    angles = tstep[0].astype(F32) * time_tab[0:1, :] + time_tab[1:2, :]
    features = sine(angles).astype(BF16)
    loads[0].wait()
    hidden = silu(one_row_dot(features, tin[...])).astype(BF16)
    loads[1].wait()
    wide = jnp.broadcast_to(hidden, (16, width))
    cond = dot_t(wide, tout[...])
    activated = silu(cond[0:1]).astype(BF16)
    loads[2].wait()
    partial = one_row_dot(activated, ada[...])
    mods[me // 2] = jnp.concatenate(
        [partial[:, :width], partial[:, width : 2 * width]], axis=0
    ).astype(BF16)
    span = gates.shape[2]
    gates[me // 2] = jnp.concatenate(
        [partial[:, 2 * width : 2 * width + span], partial[:, 3 * width - span :]], axis=0
    ).astype(BF16)
    for load in qkv_loads:
        load.start()
    ow_load = pltpu.make_async_copy(ow_h, ow, wsem.at[0])
    ow_load.start()

    pl.semaphore_wait(barrier, n - 1)

    half_n = n // 2

    @pl.loop(1, half_n)
    def _(step):
        row = me // 2
        remote(mods.at[row], mods.at[row], msend, mrecv, lax.rem(me + 2 * step, n)).start()

    norm_copies = [
        pltpu.make_async_remote_copy(
            src_ref=nsend, dst_ref=dst, send_sem=nsem.at[i], recv_sem=nrecv.at[i],
            device_id={"patch": to}, device_id_type=MESH,
        )
        for i, (dst, to) in enumerate([(ngot, mirror), (zgot, flip(me, 4)), (xgot, flip(me, 2))])
    ]
    for copy in norm_copies:
        copy.start()

    drain(mods.at[pl.ds(0, half_n - 1)], mrecv)
    partner = flip(me, 1)
    msum[...] = jnp.sum(mods[...].astype(F32), axis=0)
    sum_copy = remote(msum, mgot, hsend, hrecv, partner)
    sum_copy.start()
    sum_copy.wait_recv()
    modulation = msum[...] + mgot[...]
    shift = modulation[0:1]
    gain = 1.0 + modulation[1:2]
    modulated = (norm_s[...] * gain + shift).astype(BF16)

    lane_ids = lax.broadcasted_iota(jnp.int32, (rows, LANE), 1)

    def base_of(owner, fold_group, stride, blocks):
        lanes = lax.broadcasted_iota(jnp.int32, (fold_group, LANE), 1)
        slot = lax.broadcasted_iota(jnp.int32, (fold_group, LANE), 0)
        base = jnp.zeros((fold_group, LANE), F32)
        for r in range(rows // fold_group):
            low = r * stride + blocks * ex
            base = jnp.where(lanes == low, 1.0, base)
            bias = jnp.where(slot + r * fold_group < counts[owner], 0.0, NEG)
            base = jnp.where(lanes == low + 1, bias, base)
        return base

    def pack(parts, p, low, base, fold_group, stride, write):
        cut = p * ex
        nexts = []
        for j, part in enumerate(parts):
            here = part[:, low : low + LANE]
            after = part[:, low + LANE : low + 2 * LANE]
            nexts.append(after)
            mixed = jnp.where(lane_ids < cut, after, here)
            write(slice(j * rows, (j + 1) * rows), mixed.astype(BF16))
        packed = fold(nexts, base, fold_group, stride, ex, cut)
        write(slice(len(parts) * rows, None), packed.astype(BF16))

    def into(ref, index):
        def write(part, value):
            ref[index, part, :] = value

        return write

    def pair_parts(x, weights):
        product = dot(x, weights[...])
        parts = [product[:, i * reach : (i + 1) * reach] for i in range(3)]
        return [parts[0] * scale_q] + parts[1:]

    my_slot = group * PAIRS + pair
    slots = groups * PAIRS
    block_of = me - pair
    pltpu.make_async_copy(far_w, far_w, wsem.at[1]).wait()
    base0 = base_of(me, fold0, stride0, 3)
    parts = pair_parts(modulated, far_w)
    for q in range(2):
        pack(parts, 2 * far_chip + q, q * LANE, base0, fold0, stride0, into(sendd, q))
    for q in range(2):
        remote(sendd.at[q], got0.at[pair], dsend, drecv, block_of + 2 * far_chip + q).start()

    pltpu.make_async_copy(kv_w, kv_w, wsem.at[3]).wait()

    def kv_pack(x, owner, buffer):
        base = base_of(owner, fold1, stride1, 2)
        parts = [dot(x, kv_w[:, i * width : (i + 1) * width]) for i in range(2)]
        for p in range(PAIRS):
            pack(parts, p, p * LANE, base, fold1, stride1, into(buffer, p))

    def spread(buffer, got, send, recv, g):
        for j in range(1 if g is None else 0, PAIRS):
            turn = lax.rem(pair + j, PAIRS)
            to = (group if g is None else g) * HEADS + side * PAIRS + turn
            remote(buffer.at[turn], got.at[my_slot], send, recv, to).start()

    if groups > 1:
        kv_pack(modulated, me, send2)

        @pl.loop(1, groups)
        def _(g):
            spread(send2, got2, tsend, trecv, lax.rem(group + g, groups))

    norm_copies[0].wait_recv()
    kv_pack((ngot[...].astype(F32) * gain + shift).astype(BF16), mirror, send1)
    spread(send1, got1, rsend, rrecv, None)
    if groups > 1:

        @pl.loop(1, groups)
        def _(g):
            spread(send1, got1, rsend, rrecv, lax.rem(group + g, groups))

    got1[my_slot] = send1[pair]

    @pl.loop(1, half_n)
    def _(step):
        row = me // 2
        remote(gates.at[row], gates.at[row], gsend, grecv, lax.rem(me + 2 * step, n)).start()

    pltpu.make_async_copy(near_w, near_w, wsem.at[2]).wait()
    norm_copies[1].wait_recv()
    norm_copies[2].wait_recv()
    others = [(ref[...].astype(F32) * gain + shift).astype(BF16) for ref in (xgot, zgot)]
    parts = pair_parts(jnp.concatenate([modulated] + others, axis=0), near_w)
    owners = [pair, flip(pair, 2), flip(pair, 4)]
    bases = [base0] + [base_of(block_of + owner, fold0, stride0, 3) for owner in owners[1:]]
    mine = lax.rem(pair, 2)
    for b in range(3):
        own = [part[b * rows : (b + 1) * rows] for part in parts]
        for q in range(2):
            pack(own, 2 * chip + q, q * LANE, bases[b], fold0, stride0, into(sendp, 2 * b + q))
    for b in range(3):
        remote(sendp.at[2 * b + 1 - mine], got0.at[owners[b]], psend, precv, partner).start()
    for b in range(3):
        got0[owners[b]] = sendp[2 * b + mine]

    drain(got0.at[pl.ds(0, 3)], precv)
    drain(got0.at[pl.ds(0, 2)], drecv)

    def keys_of(got, g, first, fold_group, stride, to):
        block = got[pl.ds(g * PAIRS, PAIRS)]
        cells = PAIRS * rows
        k = block[:, first * rows : (first + 1) * rows].reshape(cells, LANE)
        v = block[:, (first + 1) * rows : (first + 2) * rows].reshape(cells, LANE)
        extra = jnp.concatenate(
            [unfold(block[s, (first + 2) * rows :].astype(F32), rows, stride, to) for s in range(PAIRS)],
            axis=0,
        ).astype(BF16)
        lanes = lax.broadcasted_iota(jnp.int32, (cells, LANE), 1)
        copies = jnp.where(lanes < ex, pltpu.roll(extra, LANE - 2 * ex, axis=1), 0.0).astype(BF16)
        step = ex
        while step < LANE:
            copies = copies + pltpu.roll(copies, step, axis=1)
            step *= 2
        return jnp.concatenate([k, extra], axis=1), jnp.concatenate([v, copies], axis=1)

    half = PAIRS // 2
    cells = half * rows
    near = pair // half
    q_lanes = lax.broadcasted_iota(jnp.int32, (cells, LANE), 1)
    column = lax.rem(q_lanes + (LANE - ex * pair), LANE)
    first_head = column < head
    bias_one = jnp.where(q_lanes == 3 * ex + 1, 1.0, 0.0)

    def queries_of(base):
        block = got0[pl.ds(base, half)]
        qa = block[:, :rows].reshape(cells, LANE).astype(F32)
        extra = jnp.concatenate(
            [
                unfold(block[s, 3 * rows :].astype(F32), rows, stride0, ex)
                for s in range(half)
            ],
            axis=0,
        )
        extra = jnp.where((q_lanes >= ex) & (q_lanes < 2 * ex), extra, bias_one)
        top = jnp.concatenate([jnp.where(first_head, qa, 0.0), bias_one], axis=1)
        low = jnp.concatenate([jnp.where(first_head, 0.0, qa), extra], axis=1)
        return jnp.concatenate([top, low], axis=0).astype(BF16)

    starts = [(1 - near) * half, near * half]
    queries = [queries_of(base) for base in starts]

    def wide(x, count):
        return jnp.concatenate([x] * count, axis=1)

    def attend(i, keys, values, first):
        scores = dot_t(queries[i], keys)
        shape = (scores.shape[0], LANE)
        top = jnp.broadcast_to(jnp.max(scores, axis=1, keepdims=True), shape)
        if not first:
            before = top_s[i]
            top = jnp.maximum(top, before)
        prob = jnp.exp2(scores - wide(top, scores.shape[1] // LANE))
        total = jnp.broadcast_to(jnp.sum(prob, axis=1, keepdims=True), shape)
        mixed = dot(prob.astype(BF16), values)
        if not first:
            decay = jnp.exp2(before - top)
            total = total_s[i] * decay + total
            mixed = o_s[i] * wide(decay, 2) + mixed
        return top, total, mixed

    def keep(i, state):
        top_s[i], total_s[i], o_s[i] = state

    keys, values = keys_of(got0, 0, 1, fold0, stride0, 0)
    for i in range(2):
        keep(i, attend(i, keys, values, True))

    if groups > 1:
        drain(got2.at[pl.ds(0, slots - PAIRS)], trecv)
    drain(got1.at[pl.ds(0, slots - 1)], rrecv)
    for g in range(1, groups):
        other = lax.rem(group + g, groups)
        for got in (got1, got2):
            keys, values = keys_of(got, other, 0, fold1, stride1, ex)
            for i in range(2):
                keep(i, attend(i, keys, values, False))

    keys, values = keys_of(got1, group, 0, fold1, stride1, ex)
    fold_zero = jnp.zeros((fold2, LANE), F32)
    fold_lanes = lax.broadcasted_iota(jnp.int32, (fold2, LANE), 1)
    for i in range(2):
        _, total, mixed = attend(i, keys, values, False)
        mixed = mixed * wide(1.0 / total, 2)
        main = jnp.where(first_head, mixed[:cells, :LANE], mixed[cells:, :LANE])
        extra = mixed[cells:, LANE:]
        for s in range(half):
            span_s = slice(s * rows, (s + 1) * rows)
            slot = starts[i] + s
            att[slot, :rows, :] = main[span_s].astype(BF16)
            packed = fold_zero
            for r in range(rows // fold2):
                low = s * rows + r * fold2
                packed = jnp.where(
                    (fold_lanes >= r * ex) & (fold_lanes < (r + 1) * ex), extra[low : low + fold2], packed
                )
            att[slot, rows:, :] = packed.astype(BF16)
        for s in range(i, half):
            slot = starts[i] + lax.rem(pair + s, half)
            remote(att.at[slot], back.at[pair], asend, arecv, me - pair + slot).start()

    drain(gates.at[pl.ds(0, half_n - 1)], grecv)
    gsum[...] = jnp.sum(gates[...].astype(F32), axis=0)
    gate_copy = remote(gsum, ggot, fsend, frecv, partner)
    gate_copy.start()
    back[pair] = att[pair]
    ow_load.wait()
    valid = (lax.broadcasted_iota(jnp.int32, (rows, 1), 0) < counts[me]).astype(F32)

    drain(mods.at[pl.ds(0, half_n - 1)], msend)
    drain(gates.at[pl.ds(0, half_n - 1)], gsend)
    sum_copy.wait_send()
    for copy in norm_copies:
        copy.wait_send()
    drain(got0.at[pl.ds(0, 2)], dsend)
    drain(got0.at[pl.ds(0, 3)], psend)
    if groups > 1:
        drain(got2.at[pl.ds(0, slots - PAIRS)], tsend)
    drain(got1.at[pl.ds(0, slots - 1)], rsend)
    drain(back.at[pl.ds(0, PAIRS - 1)], arecv)

    gate_copy.wait()
    gate_rows = gsum[...] + ggot[...]
    gate = jnp.concatenate([gate_rows[0:1], gate_rows[1:2, 2 * span - width :]], axis=1)
    rest = jnp.zeros((rows, LANE), F32)
    for p in range(PAIRS):
        piece = unfold(back[p, rows:, :].astype(F32), rows, ex, p * ex)
        rest = jnp.where((lane_ids >= p * ex) & (lane_ids < (p + 1) * ex), piece, rest)
    chunks = []
    for c in range(PAIRS + 1):
        here = back[c, :rows, :].astype(F32) if c < PAIRS else rest
        if c:
            here = jnp.where(lane_ids < c * ex, rest, here)
            here = jnp.where(lane_ids < (c - 1) * ex, back[c - 1, :rows, :].astype(F32), here)
        chunks.append(here)
    attended = jnp.concatenate(chunks, axis=1).astype(BF16)
    projected = dot(attended, ow[...])
    out[...] = (xin_s[...] + gate * projected * valid).astype(BF16)
    drain(back.at[pl.ds(0, PAIRS - 1)], asend)


def tables(width, freq):
    quarter, half = width // 4, freq // 2
    omega = np.power(10000.0, -np.arange(quarter) / quarter)
    turn = math.pi / 2
    pos_tab = np.stack([np.tile(omega, 4), np.repeat([0.0, turn, 0.0, turn], quarter)])
    wave = np.exp(-math.log(10000.0) * np.arange(half) / half)
    time_tab = np.stack([np.tile(wave, 2), np.repeat([turn, 0.0], half)])
    return pos_tab.astype(np.float32), time_tab.astype(np.float32)


def per_device(
    tokens, positions, counts, timestep, time_in, time_out, ada_weight, qkv_weight, out_weight
):
    n = lax.axis_size("patch")
    rows, width = tokens.shape
    head = width // HEADS
    ex = 2 * head - LANE
    assert 0 < ex and PAIRS * ex <= LANE and n % HEADS == 0
    size0 = 3 * rows + fold_rows(rows, 3 * ex + 2)
    size1 = 2 * rows + fold_rows(rows, 2 * ex + 2)
    size2 = rows + fold_rows(rows, ex)
    slots = n // 2
    queries = PAIRS * rows
    span = -(-width // 256) * LANE
    pos_tab, time_tab = tables(width, time_in.shape[0])
    hbm = pl.BlockSpec(memory_space=pl.ANY)
    vmem = pl.BlockSpec(memory_space=pltpu.VMEM)
    dma = pltpu.SemaphoreType.DMA
    return pl.pallas_call(
        functools.partial(block_kernel, n, rows, width, head),
        out_shape=pltpu.VMEM((rows, width), BF16),
        in_specs=[hbm] * 11,
        out_specs=vmem,
        scratch_shapes=[
            pltpu.SMEM(counts.shape, jnp.int32),
            pltpu.SMEM(timestep.shape, jnp.int32),
            pltpu.VMEM(positions.shape, jnp.int32),
            pltpu.VMEM(pos_tab.shape, F32),
            pltpu.VMEM(time_tab.shape, F32),
            pltpu.VMEM(tokens.shape, BF16),
            pltpu.VMEM(time_in.shape, BF16),
            pltpu.VMEM(time_out.shape[::-1], BF16),
            pltpu.VMEM(ada_weight.shape, BF16),
            pltpu.VMEM((width, 9 * LANE), BF16),
            pltpu.VMEM((width, 9 * LANE), BF16),
            pltpu.VMEM((width, 2 * width), BF16),
            pltpu.VMEM(out_weight.shape, BF16),
            pltpu.VMEM((n // 2, 2, width), BF16),
            pltpu.VMEM((n // 2, 2, span), BF16),
            pltpu.VMEM((2, width), F32),
            pltpu.VMEM((2, width), F32),
            pltpu.VMEM((2, span), F32),
            pltpu.VMEM((2, span), F32),
            pltpu.VMEM((rows, width), F32),
            pltpu.VMEM((rows, width), F32),
            pltpu.VMEM((rows, width), BF16),
            pltpu.VMEM((rows, width), BF16),
            pltpu.VMEM((rows, width), BF16),
            pltpu.VMEM((rows, width), BF16),
            pltpu.VMEM((2, size0, LANE), BF16),
            pltpu.VMEM((6, size0, LANE), BF16),
            pltpu.VMEM((PAIRS, size1, LANE), BF16),
            pltpu.VMEM((PAIRS, size1, LANE), BF16),
            pltpu.VMEM((PAIRS, size0, LANE), BF16),
            pltpu.VMEM((slots, size1, LANE), BF16),
            pltpu.VMEM((slots, size1, LANE), BF16),
            pltpu.VMEM((2, queries, 2 * LANE), F32),
            pltpu.VMEM((2, queries, LANE), F32),
            pltpu.VMEM((2, queries, LANE), F32),
            pltpu.VMEM((PAIRS, size2, LANE), BF16),
            pltpu.VMEM((PAIRS, size2, LANE), BF16),
            dma((5,)),
            dma((5,)),
        ]
        + [dma((4,))] + [dma((1,))] * 4 + [dma((3,))] * 2 + [dma((1,))] * 14,
        compiler_params=pltpu.CompilerParams(
            collective_id=0, has_side_effects=True, vmem_limit_bytes=60 * 2**20
        ),
    )(
        counts, timestep, positions, pos_tab, time_tab,
        tokens, time_in, time_out.T, ada_weight, qkv_weight, out_weight,
    )


def solution(mesh):
    placed = (
        P(("req", "patch"), None),
        P(None, ("req", "patch")),
        P("req"),
        P("req"),
        P(),
        P(None, "patch"),
        P("patch", None),
        P(),
        P(),
    )
    return jax.shard_map(
        per_device, mesh=mesh, in_specs=placed, out_specs=P(("req", "patch"), None), check_vma=False
    )
```

```python
import functools
import math

import jax
import jax.numpy as jnp
import numpy as np
from jax import lax
from jax.experimental import pallas as pl
from jax.experimental.pallas import tpu as pltpu
from jax.sharding import PartitionSpec as P

HEADS = 16
PAIRS = HEADS // 2
LANE = 128
NEG = -1e30
F32 = jnp.float32
BF16 = jnp.bfloat16
MESH = pl.DeviceIdType.MESH
PI_PARTS = (3.140625, 0.000967502593994140625, 1.509957990978376432e-07)


def silu(v):
    return v / (1.0 + jnp.exp(-v))


def sine(x):
    turns = jnp.floor(x * (1.0 / math.pi) + 0.5)
    r = x - turns * PI_PARTS[0]
    r = r - turns * PI_PARTS[1]
    r = r - turns * PI_PARTS[2]
    s = r * r
    poly = -2.3889859e-08 * s + 2.7525562e-06
    poly = poly * s - 0.00019840874
    poly = poly * s + 0.0083333310
    poly = poly * s - 0.16666667
    value = r + r * (s * poly)
    odd = turns - 2.0 * jnp.floor(turns * 0.5)
    return value * (1.0 - 2.0 * odd)


def dot(a, b):
    return jnp.dot(a, b, preferred_element_type=F32)


def dot_t(a, b):
    return lax.dot_general(a, b, (((1,), (1,)), ((), ())), preferred_element_type=F32)


def one_row_dot(row, matrix):
    wide = jnp.broadcast_to(row, (16, row.shape[1])).astype(BF16)
    return dot(wide, matrix)[0:1]


def fold_rows(rows, stride):
    group = 8
    while rows % group or rows // group * stride > LANE:
        group += 8
    return group


def turned(x, shift):
    if isinstance(shift, int):
        shift %= LANE
        return pltpu.roll(x, shift, axis=1) if shift else x
    return pltpu.roll(x, lax.rem(shift + LANE, LANE), axis=1)


def flip(index, bit):
    return index + bit * (1 - 2 * lax.rem(index // bit, 2))


def fold(blocks, base, group, stride, ex, at):
    lanes = lax.broadcasted_iota(jnp.int32, (group, LANE), 1)
    packed = base
    for r in range(blocks[0].shape[0] // group):
        for j, block in enumerate(blocks):
            low = r * stride + j * ex
            piece = turned(block[r * group : (r + 1) * group], low - at)
            packed = jnp.where((lanes >= low) & (lanes < low + ex), piece, packed)
    return packed


def unfold(packed, rows, stride, to):
    group = packed.shape[0]
    return jnp.concatenate(
        [turned(packed, to - r * stride) for r in range(rows // group)], axis=0
    )


def block_kernel(
    n, rows, width, head,
    counts_h, tstep_h, pos_h, pos_tab_h, time_tab_h,
    tok_h, tin_h, tout_h, ada_h, qkv_h, ow_h,
    out,
    counts, tstep, pos, pos_tab, time_tab, tok, tin, tout, ada, near_w, far_w, kv_w, ow,
    mods, gates, msum, gsum, xin_s, norm_s, nsend, ngot, xgot, zgot, sendd, sendp, send1, send2,
    got0, got1, got2, o_s, top_s, total_s, att, back,
    lsem, ssem, wsem, msend, mrecv, gsend, grecv, nsem, nrecv, dsend, drecv, psend, precv,
    rsend, rrecv, tsend, trecv, asend, arecv, hsend, hrecv, fsend, frecv,
):
    me = lax.axis_index("patch")
    pair = lax.rem(me, PAIRS)
    side = lax.rem(me // PAIRS, 2)
    group = me // HEADS
    groups = n // HEADS
    mirror = flip(flip(me, PAIRS), PAIRS // 2)
    ex = 2 * head - LANE
    stride0, stride1 = 3 * ex + 2, 2 * ex + 2
    fold0, fold1, fold2 = fold_rows(rows, stride0), fold_rows(rows, stride1), fold_rows(rows, ex)
    scale_q = math.log2(math.e) / math.sqrt(head)

    barrier = pltpu.get_barrier_semaphore()

    def drain(ref, sem):
        pltpu.make_async_copy(ref, ref, sem.at[0]).wait()

    def remote(src, dst, send, recv, to):
        return pltpu.make_async_remote_copy(
            src_ref=src, dst_ref=dst, send_sem=send.at[0], recv_sem=recv.at[0],
            device_id={"patch": to}, device_id_type=MESH,
        )

    @pl.loop(1, n)
    def _(step):
        pl.semaphore_signal(
            barrier, inc=1, device_id={"patch": lax.rem(me + step, n)}, device_id_type=MESH
        )

    loads = [
        pltpu.make_async_copy(src, dst, lsem.at[i])
        for i, (src, dst) in enumerate(
            [(tin_h, tin), (tout_h, tout), (ada_h, ada), (tok_h, tok)]
        )
    ]
    chip = pair // 2
    far_chip = flip(flip(pair, 2), 4) // 2
    reach = near_w.shape[1] // 3

    def window(i, owner):
        return pl.ds(pl.multiple_of(i * width + 2 * LANE * owner, LANE), reach)

    qkv_loads = [
        pltpu.make_async_copy(
            qkv_h.at[:, window(i, owner)], dst.at[:, pl.ds(i * reach, reach)], wsem.at[k]
        )
        for k, (owner, dst) in ((1, (far_chip, far_w)), (2, (chip, near_w)))
        for i in range(3)
    ]
    qkv_loads.insert(3, pltpu.make_async_copy(qkv_h.at[:, pl.ds(width, 2 * width)], kv_w, wsem.at[3]))
    small = [
        pltpu.make_async_copy(src, dst, ssem.at[i])
        for i, (src, dst) in enumerate(
            [(tstep_h, tstep), (time_tab_h, time_tab), (counts_h, counts),
             (pos_h, pos), (pos_tab_h, pos_tab)]
        )
    ]
    for load in small[2:] + loads[3:] + small[:2] + loads[:3]:
        load.start()

    ids = lax.broadcasted_iota(jnp.int32, (rows, rows), 0)
    eye = ids == lax.broadcasted_iota(jnp.int32, (rows, rows), 1)
    for load in small[2:]:
        load.wait()
    posf = pos[...].astype(F32)
    row_col = jnp.sum(jnp.where(eye, posf[0:1, :], 0.0), axis=1, keepdims=True)
    col_col = jnp.sum(jnp.where(eye, posf[1:2, :], 0.0), axis=1, keepdims=True)
    wide_lanes = lax.broadcasted_iota(jnp.int32, (1, width), 1)
    place = jnp.where(wide_lanes < width // 2, row_col, col_col)
    embed = sine(place * pos_tab[0:1, :] + pos_tab[1:2, :])
    loads[3].wait()
    x_in = tok[...].astype(F32) + embed
    xin_s[...] = x_in
    centered = x_in - jnp.mean(x_in, axis=1, keepdims=True)
    variance = jnp.mean(centered * centered, axis=1, keepdims=True)
    norm = centered * lax.rsqrt(variance + 1e-6)
    norm_s[...] = norm
    nsend[...] = norm.astype(BF16)
    for load in small[:2]:
        load.wait()
    angles = tstep[0].astype(F32) * time_tab[0:1, :] + time_tab[1:2, :]
    features = sine(angles).astype(BF16)
    loads[0].wait()
    hidden = silu(one_row_dot(features, tin[...])).astype(BF16)
    loads[1].wait()
    wide = jnp.broadcast_to(hidden, (16, width))
    cond = dot_t(wide, tout[...])
    activated = silu(cond[0:1]).astype(BF16)
    loads[2].wait()
    partial = one_row_dot(activated, ada[...])
    mods[me] = jnp.concatenate(
        [partial[:, :width], partial[:, width : 2 * width]], axis=0
    ).astype(BF16)
    span = gates.shape[2]
    gates[me] = jnp.concatenate(
        [partial[:, 2 * width : 2 * width + span], partial[:, 3 * width - span :]], axis=0
    ).astype(BF16)
    for load in qkv_loads:
        load.start()
    ow_load = pltpu.make_async_copy(ow_h, ow, wsem.at[0])
    ow_load.start()

    pl.semaphore_wait(barrier, n - 1)

    core = lax.rem(me, 2)
    partner = flip(me, 1)
    half_n = n // 2

    def to_odd(ref, send, recv):
        @pl.loop(1, half_n)
        def _(step):
            to = 2 * lax.rem(me // 2 + step, half_n) + 1
            remote(ref.at[me], ref.at[me], send, recv, to).start()

        @pl.when(core == 0)
        def _():
            remote(ref.at[me], ref.at[me], send, recv, partner).start()

    def total_of(ref, total, recv, send, done):
        @pl.when(core == 1)
        def _():
            drain(ref.at[pl.ds(0, n - 1)], recv)
            total[...] = jnp.sum(ref[...].astype(F32), axis=0)
            remote(total, total, send, done, partner).start()

    def sent(ref, send):
        @pl.when(core == 0)
        def _():
            drain(ref.at[pl.ds(0, half_n)], send)

        @pl.when(core == 1)
        def _():
            drain(ref.at[pl.ds(0, half_n - 1)], send)

    to_odd(mods, msend, mrecv)

    norm_copies = [
        pltpu.make_async_remote_copy(
            src_ref=nsend, dst_ref=dst, send_sem=nsem.at[i], recv_sem=nrecv.at[i],
            device_id={"patch": to}, device_id_type=MESH,
        )
        for i, (dst, to) in enumerate([(ngot, mirror), (zgot, flip(me, 4)), (xgot, flip(me, 2))])
    ]
    for copy in norm_copies:
        copy.start()

    total_of(mods, msum, mrecv, hsend, hrecv)

    @pl.when(core == 0)
    def _():
        drain(msum, hrecv)

    modulation = msum[...]
    shift = modulation[0:1]
    gain = 1.0 + modulation[1:2]
    modulated = (norm_s[...] * gain + shift).astype(BF16)

    lane_ids = lax.broadcasted_iota(jnp.int32, (rows, LANE), 1)

    def base_of(owner, fold_group, stride, blocks):
        lanes = lax.broadcasted_iota(jnp.int32, (fold_group, LANE), 1)
        slot = lax.broadcasted_iota(jnp.int32, (fold_group, LANE), 0)
        base = jnp.zeros((fold_group, LANE), F32)
        for r in range(rows // fold_group):
            low = r * stride + blocks * ex
            base = jnp.where(lanes == low, 1.0, base)
            bias = jnp.where(slot + r * fold_group < counts[owner], 0.0, NEG)
            base = jnp.where(lanes == low + 1, bias, base)
        return base

    def pack(parts, p, low, base, fold_group, stride, write):
        cut = p * ex
        nexts = []
        for j, part in enumerate(parts):
            here = part[:, low : low + LANE]
            after = part[:, low + LANE : low + 2 * LANE]
            nexts.append(after)
            mixed = jnp.where(lane_ids < cut, after, here)
            write(slice(j * rows, (j + 1) * rows), mixed.astype(BF16))
        packed = fold(nexts, base, fold_group, stride, ex, cut)
        write(slice(len(parts) * rows, None), packed.astype(BF16))

    def into(ref, index):
        def write(part, value):
            ref[index, part, :] = value

        return write

    def pair_parts(x, weights):
        product = dot(x, weights[...])
        parts = [product[:, i * reach : (i + 1) * reach] for i in range(3)]
        return [parts[0] * scale_q] + parts[1:]

    my_slot = group * PAIRS + pair
    slots = groups * PAIRS
    block_of = me - pair
    pltpu.make_async_copy(far_w, far_w, wsem.at[1]).wait()
    base0 = base_of(me, fold0, stride0, 3)
    parts = pair_parts(modulated, far_w)
    for q in range(2):
        pack(parts, 2 * far_chip + q, q * LANE, base0, fold0, stride0, into(sendd, q))
    for q in range(2):
        remote(sendd.at[q], got0.at[pair], dsend, drecv, block_of + 2 * far_chip + q).start()

    pltpu.make_async_copy(kv_w, kv_w, wsem.at[3]).wait()

    def kv_pack(x, owner, buffer):
        base = base_of(owner, fold1, stride1, 2)
        parts = [dot(x, kv_w[:, i * width : (i + 1) * width]) for i in range(2)]
        for p in range(PAIRS):
            pack(parts, p, p * LANE, base, fold1, stride1, into(buffer, p))

    def spread(buffer, got, send, recv, g):
        for j in range(1 if g is None else 0, PAIRS):
            turn = lax.rem(pair + j, PAIRS)
            to = (group if g is None else g) * HEADS + side * PAIRS + turn
            remote(buffer.at[turn], got.at[my_slot], send, recv, to).start()

    if groups > 1:
        kv_pack(modulated, me, send2)

        @pl.loop(1, groups)
        def _(g):
            spread(send2, got2, tsend, trecv, lax.rem(group + g, groups))

    norm_copies[0].wait_recv()
    kv_pack((ngot[...].astype(F32) * gain + shift).astype(BF16), mirror, send1)
    spread(send1, got1, rsend, rrecv, None)
    if groups > 1:

        @pl.loop(1, groups)
        def _(g):
            spread(send1, got1, rsend, rrecv, lax.rem(group + g, groups))

    got1[my_slot] = send1[pair]

    to_odd(gates, gsend, grecv)

    pltpu.make_async_copy(near_w, near_w, wsem.at[2]).wait()
    norm_copies[1].wait_recv()
    norm_copies[2].wait_recv()
    others = [(ref[...].astype(F32) * gain + shift).astype(BF16) for ref in (xgot, zgot)]
    parts = pair_parts(jnp.concatenate([modulated] + others, axis=0), near_w)
    owners = [pair, flip(pair, 2), flip(pair, 4)]
    bases = [base0] + [base_of(block_of + owner, fold0, stride0, 3) for owner in owners[1:]]
    mine = lax.rem(pair, 2)
    for b in range(3):
        own = [part[b * rows : (b + 1) * rows] for part in parts]
        for q in range(2):
            pack(own, 2 * chip + q, q * LANE, bases[b], fold0, stride0, into(sendp, 2 * b + q))
    for b in range(3):
        remote(sendp.at[2 * b + 1 - mine], got0.at[owners[b]], psend, precv, partner).start()
    for b in range(3):
        got0[owners[b]] = sendp[2 * b + mine]

    drain(got0.at[pl.ds(0, 3)], precv)
    drain(got0.at[pl.ds(0, 2)], drecv)

    def keys_of(got, g, first, fold_group, stride, to):
        block = got[pl.ds(g * PAIRS, PAIRS)]
        cells = PAIRS * rows
        k = block[:, first * rows : (first + 1) * rows].reshape(cells, LANE)
        v = block[:, (first + 1) * rows : (first + 2) * rows].reshape(cells, LANE)
        extra = jnp.concatenate(
            [unfold(block[s, (first + 2) * rows :].astype(F32), rows, stride, to) for s in range(PAIRS)],
            axis=0,
        ).astype(BF16)
        lanes = lax.broadcasted_iota(jnp.int32, (cells, LANE), 1)
        copies = jnp.where(lanes < ex, pltpu.roll(extra, LANE - 2 * ex, axis=1), 0.0).astype(BF16)
        step = ex
        while step < LANE:
            copies = copies + pltpu.roll(copies, step, axis=1)
            step *= 2
        return jnp.concatenate([k, extra], axis=1), jnp.concatenate([v, copies], axis=1)

    half = PAIRS // 2
    cells = half * rows
    near = pair // half
    q_lanes = lax.broadcasted_iota(jnp.int32, (cells, LANE), 1)
    column = lax.rem(q_lanes + (LANE - ex * pair), LANE)
    first_head = column < head
    bias_one = jnp.where(q_lanes == 3 * ex + 1, 1.0, 0.0)

    def queries_of(base):
        block = got0[pl.ds(base, half)]
        qa = block[:, :rows].reshape(cells, LANE).astype(F32)
        extra = jnp.concatenate(
            [
                unfold(block[s, 3 * rows :].astype(F32), rows, stride0, ex)
                for s in range(half)
            ],
            axis=0,
        )
        extra = jnp.where((q_lanes >= ex) & (q_lanes < 2 * ex), extra, bias_one)
        top = jnp.concatenate([jnp.where(first_head, qa, 0.0), bias_one], axis=1)
        low = jnp.concatenate([jnp.where(first_head, 0.0, qa), extra], axis=1)
        return jnp.concatenate([top, low], axis=0).astype(BF16)

    starts = [(1 - near) * half, near * half]
    queries = [queries_of(base) for base in starts]

    def wide(x, count):
        return jnp.concatenate([x] * count, axis=1)

    def attend(i, keys, values, first):
        scores = dot_t(queries[i], keys)
        shape = (scores.shape[0], LANE)
        top = jnp.broadcast_to(jnp.max(scores, axis=1, keepdims=True), shape)
        if not first:
            before = top_s[i]
            top = jnp.maximum(top, before)
        prob = jnp.exp2(scores - wide(top, scores.shape[1] // LANE))
        total = jnp.broadcast_to(jnp.sum(prob, axis=1, keepdims=True), shape)
        mixed = dot(prob.astype(BF16), values)
        if not first:
            decay = jnp.exp2(before - top)
            total = total_s[i] * decay + total
            mixed = o_s[i] * wide(decay, 2) + mixed
        return top, total, mixed

    def keep(i, state):
        top_s[i], total_s[i], o_s[i] = state

    keys, values = keys_of(got0, 0, 1, fold0, stride0, 0)
    for i in range(2):
        keep(i, attend(i, keys, values, True))

    if groups > 1:
        drain(got2.at[pl.ds(0, slots - PAIRS)], trecv)
    drain(got1.at[pl.ds(0, slots - 1)], rrecv)
    for g in range(1, groups):
        other = lax.rem(group + g, groups)
        for got in (got1, got2):
            keys, values = keys_of(got, other, 0, fold1, stride1, ex)
            for i in range(2):
                keep(i, attend(i, keys, values, False))

    keys, values = keys_of(got1, group, 0, fold1, stride1, ex)
    fold_zero = jnp.zeros((fold2, LANE), F32)
    fold_lanes = lax.broadcasted_iota(jnp.int32, (fold2, LANE), 1)
    for i in range(2):
        _, total, mixed = attend(i, keys, values, False)
        mixed = mixed * wide(1.0 / total, 2)
        main = jnp.where(first_head, mixed[:cells, :LANE], mixed[cells:, :LANE])
        extra = mixed[cells:, LANE:]
        for s in range(half):
            span_s = slice(s * rows, (s + 1) * rows)
            slot = starts[i] + s
            att[slot, :rows, :] = main[span_s].astype(BF16)
            packed = fold_zero
            for r in range(rows // fold2):
                low = s * rows + r * fold2
                packed = jnp.where(
                    (fold_lanes >= r * ex) & (fold_lanes < (r + 1) * ex), extra[low : low + fold2], packed
                )
            att[slot, rows:, :] = packed.astype(BF16)
        for s in range(i, half):
            slot = starts[i] + lax.rem(pair + s, half)
            remote(att.at[slot], back.at[pair], asend, arecv, me - pair + slot).start()

    total_of(gates, gsum, grecv, fsend, frecv)
    back[pair] = att[pair]
    ow_load.wait()
    valid = (lax.broadcasted_iota(jnp.int32, (rows, 1), 0) < counts[me]).astype(F32)

    sent(mods, msend)
    sent(gates, gsend)

    @pl.when(core == 1)
    def _():
        drain(msum, hsend)

    for copy in norm_copies:
        copy.wait_send()
    drain(got0.at[pl.ds(0, 2)], dsend)
    drain(got0.at[pl.ds(0, 3)], psend)
    if groups > 1:
        drain(got2.at[pl.ds(0, slots - PAIRS)], tsend)
    drain(got1.at[pl.ds(0, slots - 1)], rsend)
    drain(back.at[pl.ds(0, PAIRS - 1)], arecv)


    @pl.when(core == 1)
    def _():
        drain(gsum, fsend)

    @pl.when(core == 0)
    def _():
        drain(gsum, frecv)

    gate_rows = gsum[...]
    gate = jnp.concatenate([gate_rows[0:1], gate_rows[1:2, 2 * span - width :]], axis=1)
    rest = jnp.zeros((rows, LANE), F32)
    for p in range(PAIRS):
        piece = unfold(back[p, rows:, :].astype(F32), rows, ex, p * ex)
        rest = jnp.where((lane_ids >= p * ex) & (lane_ids < (p + 1) * ex), piece, rest)
    chunks = []
    for c in range(PAIRS + 1):
        here = back[c, :rows, :].astype(F32) if c < PAIRS else rest
        if c:
            here = jnp.where(lane_ids < c * ex, rest, here)
            here = jnp.where(lane_ids < (c - 1) * ex, back[c - 1, :rows, :].astype(F32), here)
        chunks.append(here)
    attended = jnp.concatenate(chunks, axis=1).astype(BF16)
    projected = dot(attended, ow[...])
    out[...] = (xin_s[...] + gate * projected * valid).astype(BF16)
    drain(back.at[pl.ds(0, PAIRS - 1)], asend)


def tables(width, freq):
    quarter, half = width // 4, freq // 2
    omega = np.power(10000.0, -np.arange(quarter) / quarter)
    turn = math.pi / 2
    pos_tab = np.stack([np.tile(omega, 4), np.repeat([0.0, turn, 0.0, turn], quarter)])
    wave = np.exp(-math.log(10000.0) * np.arange(half) / half)
    time_tab = np.stack([np.tile(wave, 2), np.repeat([turn, 0.0], half)])
    return pos_tab.astype(np.float32), time_tab.astype(np.float32)


def per_device(
    tokens, positions, counts, timestep, time_in, time_out, ada_weight, qkv_weight, out_weight
):
    n = lax.axis_size("patch")
    rows, width = tokens.shape
    head = width // HEADS
    ex = 2 * head - LANE
    assert 0 < ex and PAIRS * ex <= LANE and n % HEADS == 0
    size0 = 3 * rows + fold_rows(rows, 3 * ex + 2)
    size1 = 2 * rows + fold_rows(rows, 2 * ex + 2)
    size2 = rows + fold_rows(rows, ex)
    slots = n // 2
    queries = PAIRS * rows
    span = -(-width // 256) * LANE
    pos_tab, time_tab = tables(width, time_in.shape[0])
    hbm = pl.BlockSpec(memory_space=pl.ANY)
    vmem = pl.BlockSpec(memory_space=pltpu.VMEM)
    dma = pltpu.SemaphoreType.DMA
    return pl.pallas_call(
        functools.partial(block_kernel, n, rows, width, head),
        out_shape=pltpu.VMEM((rows, width), BF16),
        in_specs=[hbm] * 11,
        out_specs=vmem,
        scratch_shapes=[
            pltpu.SMEM(counts.shape, jnp.int32),
            pltpu.SMEM(timestep.shape, jnp.int32),
            pltpu.VMEM(positions.shape, jnp.int32),
            pltpu.VMEM(pos_tab.shape, F32),
            pltpu.VMEM(time_tab.shape, F32),
            pltpu.VMEM(tokens.shape, BF16),
            pltpu.VMEM(time_in.shape, BF16),
            pltpu.VMEM(time_out.shape[::-1], BF16),
            pltpu.VMEM(ada_weight.shape, BF16),
            pltpu.VMEM((width, 9 * LANE), BF16),
            pltpu.VMEM((width, 9 * LANE), BF16),
            pltpu.VMEM((width, 2 * width), BF16),
            pltpu.VMEM(out_weight.shape, BF16),
            pltpu.VMEM((n, 2, width), BF16),
            pltpu.VMEM((n, 2, span), BF16),
            pltpu.VMEM((2, width), F32),
            pltpu.VMEM((2, span), F32),
            pltpu.VMEM((rows, width), F32),
            pltpu.VMEM((rows, width), F32),
            pltpu.VMEM((rows, width), BF16),
            pltpu.VMEM((rows, width), BF16),
            pltpu.VMEM((rows, width), BF16),
            pltpu.VMEM((rows, width), BF16),
            pltpu.VMEM((2, size0, LANE), BF16),
            pltpu.VMEM((6, size0, LANE), BF16),
            pltpu.VMEM((PAIRS, size1, LANE), BF16),
            pltpu.VMEM((PAIRS, size1, LANE), BF16),
            pltpu.VMEM((PAIRS, size0, LANE), BF16),
            pltpu.VMEM((slots, size1, LANE), BF16),
            pltpu.VMEM((slots, size1, LANE), BF16),
            pltpu.VMEM((2, queries, 2 * LANE), F32),
            pltpu.VMEM((2, queries, LANE), F32),
            pltpu.VMEM((2, queries, LANE), F32),
            pltpu.VMEM((PAIRS, size2, LANE), BF16),
            pltpu.VMEM((PAIRS, size2, LANE), BF16),
            dma((5,)),
            dma((5,)),
        ]
        + [dma((4,))] + [dma((1,))] * 4 + [dma((3,))] * 2 + [dma((1,))] * 14,
        compiler_params=pltpu.CompilerParams(
            collective_id=0, has_side_effects=True, vmem_limit_bytes=60 * 2**20
        ),
    )(
        counts, timestep, positions, pos_tab, time_tab,
        tokens, time_in, time_out.T, ada_weight, qkv_weight, out_weight,
    )


def solution(mesh):
    placed = (
        P(("req", "patch"), None),
        P(None, ("req", "patch")),
        P("req"),
        P("req"),
        P(),
        P(None, "patch"),
        P("patch", None),
        P(),
        P(),
    )
    return jax.shard_map(
        per_device, mesh=mesh, in_specs=placed, out_specs=P(("req", "patch"), None), check_vma=False
    )
```

```python
import functools
import math

import jax
import jax.numpy as jnp
import numpy as np
from jax import lax
from jax.experimental import pallas as pl
from jax.experimental.pallas import tpu as pltpu
from jax.sharding import PartitionSpec as P

HEADS = 16
PAIRS = HEADS // 2
LANE = 128
NEG = -1e30
F32 = jnp.float32
BF16 = jnp.bfloat16
MESH = pl.DeviceIdType.MESH
PI_PARTS = (3.140625, 0.000967502593994140625, 1.509957990978376432e-07)


def silu(v):
    return v / (1.0 + jnp.exp(-v))


def sine(x):
    turns = jnp.floor(x * (1.0 / math.pi) + 0.5)
    r = x - turns * PI_PARTS[0]
    r = r - turns * PI_PARTS[1]
    r = r - turns * PI_PARTS[2]
    s = r * r
    poly = -2.3889859e-08 * s + 2.7525562e-06
    poly = poly * s - 0.00019840874
    poly = poly * s + 0.0083333310
    poly = poly * s - 0.16666667
    value = r + r * (s * poly)
    odd = turns - 2.0 * jnp.floor(turns * 0.5)
    return value * (1.0 - 2.0 * odd)


def dot(a, b):
    return jnp.dot(a, b, preferred_element_type=F32)


def dot_t(a, b):
    return lax.dot_general(a, b, (((1,), (1,)), ((), ())), preferred_element_type=F32)


def one_row_dot(row, matrix):
    wide = jnp.broadcast_to(row, (16, row.shape[1])).astype(BF16)
    return dot(wide, matrix)[0:1]


def fold_rows(rows, stride):
    group = 8
    while rows % group or rows // group * stride > LANE:
        group += 8
    return group


def turned(x, shift):
    if isinstance(shift, int):
        shift %= LANE
        return pltpu.roll(x, shift, axis=1) if shift else x
    return pltpu.roll(x, lax.rem(shift + LANE, LANE), axis=1)


def flip(index, bit):
    return index + bit * (1 - 2 * lax.rem(index // bit, 2))


def fold(blocks, base, group, stride, ex, at):
    lanes = lax.broadcasted_iota(jnp.int32, (group, LANE), 1)
    packed = base
    for r in range(blocks[0].shape[0] // group):
        for j, block in enumerate(blocks):
            low = r * stride + j * ex
            piece = turned(block[r * group : (r + 1) * group], low - at)
            packed = jnp.where((lanes >= low) & (lanes < low + ex), piece, packed)
    return packed


def unfold(packed, rows, stride, to):
    group = packed.shape[0]
    return jnp.concatenate(
        [turned(packed, to - r * stride) for r in range(rows // group)], axis=0
    )


def block_kernel(
    n, rows, width, head,
    counts_h, tstep_h, pos_h, pos_tab_h, time_tab_h,
    tok_h, tin_h, tout_h, ada_h, qkv_h, ow_h,
    out,
    counts, tstep, pos, pos_tab, time_tab, tok, tin, tout, ada, near_w, far_w, kv_w, ow,
    mods, gates, msum, gsum, xin_s, norm_s, nsend, ngot, xgot, zgot, sendd, sendp, send1, send2,
    got0, got1, got2, o_s, top_s, total_s, att, back,
    lsem, ssem, wsem, msend, mrecv, gsend, grecv, nsem, nrecv, dsend, drecv, psend, precv,
    rsend, rrecv, tsend, trecv, asend, arecv, hsend, hrecv, fsend, frecv,
):
    me = lax.axis_index("patch")
    pair = lax.rem(me, PAIRS)
    side = lax.rem(me // PAIRS, 2)
    group = me // HEADS
    groups = n // HEADS
    mirror = flip(flip(me, PAIRS), PAIRS // 2)
    ex = 2 * head - LANE
    stride0, stride1 = 3 * ex + 2, 2 * ex + 2
    fold0, fold1, fold2 = fold_rows(rows, stride0), fold_rows(rows, stride1), fold_rows(rows, ex)
    scale_q = math.log2(math.e) / math.sqrt(head)

    barrier = pltpu.get_barrier_semaphore()

    def drain(ref, sem):
        pltpu.make_async_copy(ref, ref, sem.at[0]).wait()

    def remote(src, dst, send, recv, to):
        return pltpu.make_async_remote_copy(
            src_ref=src, dst_ref=dst, send_sem=send.at[0], recv_sem=recv.at[0],
            device_id={"patch": to}, device_id_type=MESH,
        )

    def greet(to):
        pl.semaphore_signal(barrier, inc=1, device_id={"patch": to}, device_id_type=MESH)

    loads = [
        pltpu.make_async_copy(src, dst, lsem.at[i])
        for i, (src, dst) in enumerate(
            [(tin_h, tin), (tout_h, tout), (ada_h, ada), (tok_h, tok)]
        )
    ]
    chip = pair // 2
    far_chip = flip(flip(pair, 2), 4) // 2
    reach = near_w.shape[1] // 3

    def window(i, owner):
        return pl.ds(pl.multiple_of(i * width + 2 * LANE * owner, LANE), reach)

    qkv_loads = [
        pltpu.make_async_copy(
            qkv_h.at[:, window(i, owner)], dst.at[:, pl.ds(i * reach, reach)], wsem.at[k]
        )
        for k, (owner, dst) in ((1, (far_chip, far_w)), (2, (chip, near_w)))
        for i in range(3)
    ]
    qkv_loads.insert(3, pltpu.make_async_copy(qkv_h.at[:, pl.ds(width, 2 * width)], kv_w, wsem.at[3]))
    small = [
        pltpu.make_async_copy(src, dst, ssem.at[i])
        for i, (src, dst) in enumerate(
            [(tstep_h, tstep), (time_tab_h, time_tab), (counts_h, counts),
             (pos_h, pos), (pos_tab_h, pos_tab)]
        )
    ]
    for load in small[2:] + loads[3:] + small[:2] + loads[:3]:
        load.start()

    @pl.when(lax.rem(me, 2) == 1)
    def _():
        @pl.loop(1, n)
        def _(step):
            greet(lax.rem(me + step, n))

    @pl.when(lax.rem(me, 2) == 0)
    def _():
        greet(mirror)

        @pl.loop(1, n // 2)
        def _(step):
            turn = lax.rem(me // HEADS * PAIRS + pair + step, n // 2)
            greet(turn // PAIRS * HEADS + side * PAIRS + lax.rem(turn, PAIRS))


    ids = lax.broadcasted_iota(jnp.int32, (rows, rows), 0)
    eye = ids == lax.broadcasted_iota(jnp.int32, (rows, rows), 1)
    for load in small[2:]:
        load.wait()
    posf = pos[...].astype(F32)
    row_col = jnp.sum(jnp.where(eye, posf[0:1, :], 0.0), axis=1, keepdims=True)
    col_col = jnp.sum(jnp.where(eye, posf[1:2, :], 0.0), axis=1, keepdims=True)
    wide_lanes = lax.broadcasted_iota(jnp.int32, (1, width), 1)
    place = jnp.where(wide_lanes < width // 2, row_col, col_col)
    embed = sine(place * pos_tab[0:1, :] + pos_tab[1:2, :])
    loads[3].wait()
    x_in = tok[...].astype(F32) + embed
    xin_s[...] = x_in
    centered = x_in - jnp.mean(x_in, axis=1, keepdims=True)
    variance = jnp.mean(centered * centered, axis=1, keepdims=True)
    norm = centered * lax.rsqrt(variance + 1e-6)
    norm_s[...] = norm
    nsend[...] = norm.astype(BF16)
    for load in small[:2]:
        load.wait()
    angles = tstep[0].astype(F32) * time_tab[0:1, :] + time_tab[1:2, :]
    features = sine(angles).astype(BF16)
    loads[0].wait()
    hidden = silu(one_row_dot(features, tin[...])).astype(BF16)
    loads[1].wait()
    wide = jnp.broadcast_to(hidden, (16, width))
    cond = dot_t(wide, tout[...])
    activated = silu(cond[0:1]).astype(BF16)
    loads[2].wait()
    partial = one_row_dot(activated, ada[...])
    mods[me] = jnp.concatenate(
        [partial[:, :width], partial[:, width : 2 * width]], axis=0
    ).astype(BF16)
    span = gates.shape[2]
    gates[me] = jnp.concatenate(
        [partial[:, 2 * width : 2 * width + span], partial[:, 3 * width - span :]], axis=0
    ).astype(BF16)
    for load in qkv_loads:
        load.start()
    ow_load = pltpu.make_async_copy(ow_h, ow, wsem.at[0])
    ow_load.start()


    @pl.when(lax.rem(me, 2) == 1)
    def _():
        pl.semaphore_wait(barrier, n // 4 * 3 - 1)

    @pl.when(lax.rem(me, 2) == 0)
    def _():
        pl.semaphore_wait(barrier, n // 4 * 3)


    core = lax.rem(me, 2)
    partner = flip(me, 1)
    half_n = n // 2

    def to_odd(ref, send, recv):
        @pl.loop(1, half_n)
        def _(step):
            to = 2 * lax.rem(me // 2 + step, half_n) + 1
            remote(ref.at[me], ref.at[me], send, recv, to).start()

        @pl.when(core == 0)
        def _():
            remote(ref.at[me], ref.at[me], send, recv, partner).start()

    def total_of(ref, total, recv, send, done):
        @pl.when(core == 1)
        def _():
            drain(ref.at[pl.ds(0, n - 1)], recv)
            total[...] = jnp.sum(ref[...].astype(F32), axis=0)
            remote(total, total, send, done, partner).start()

    def sent(ref, send):
        @pl.when(core == 0)
        def _():
            drain(ref.at[pl.ds(0, half_n)], send)

        @pl.when(core == 1)
        def _():
            drain(ref.at[pl.ds(0, half_n - 1)], send)

    to_odd(mods, msend, mrecv)

    norm_copies = [
        pltpu.make_async_remote_copy(
            src_ref=nsend, dst_ref=dst, send_sem=nsem.at[i], recv_sem=nrecv.at[i],
            device_id={"patch": to}, device_id_type=MESH,
        )
        for i, (dst, to) in enumerate([(ngot, mirror), (zgot, flip(me, 4)), (xgot, flip(me, 2))])
    ]
    for copy in norm_copies:
        copy.start()

    total_of(mods, msum, mrecv, hsend, hrecv)

    @pl.when(core == 0)
    def _():
        drain(msum, hrecv)

    modulation = msum[...]
    shift = modulation[0:1]
    gain = 1.0 + modulation[1:2]
    modulated = (norm_s[...] * gain + shift).astype(BF16)

    lane_ids = lax.broadcasted_iota(jnp.int32, (rows, LANE), 1)

    def base_of(owner, fold_group, stride, blocks):
        lanes = lax.broadcasted_iota(jnp.int32, (fold_group, LANE), 1)
        slot = lax.broadcasted_iota(jnp.int32, (fold_group, LANE), 0)
        base = jnp.zeros((fold_group, LANE), F32)
        for r in range(rows // fold_group):
            low = r * stride + blocks * ex
            base = jnp.where(lanes == low, 1.0, base)
            bias = jnp.where(slot + r * fold_group < counts[owner], 0.0, NEG)
            base = jnp.where(lanes == low + 1, bias, base)
        return base

    def pack(parts, p, low, base, fold_group, stride, write):
        cut = p * ex
        nexts = []
        for j, part in enumerate(parts):
            here = part[:, low : low + LANE]
            after = part[:, low + LANE : low + 2 * LANE]
            nexts.append(after)
            mixed = jnp.where(lane_ids < cut, after, here)
            write(slice(j * rows, (j + 1) * rows), mixed.astype(BF16))
        packed = fold(nexts, base, fold_group, stride, ex, cut)
        write(slice(len(parts) * rows, None), packed.astype(BF16))

    def into(ref, index):
        def write(part, value):
            ref[index, part, :] = value

        return write

    def pair_parts(x, weights):
        product = dot(x, weights[...])
        parts = [product[:, i * reach : (i + 1) * reach] for i in range(3)]
        return [parts[0] * scale_q] + parts[1:]

    my_slot = group * PAIRS + pair
    slots = groups * PAIRS
    block_of = me - pair
    pltpu.make_async_copy(far_w, far_w, wsem.at[1]).wait()
    base0 = base_of(me, fold0, stride0, 3)
    parts = pair_parts(modulated, far_w)
    for q in range(2):
        pack(parts, 2 * far_chip + q, q * LANE, base0, fold0, stride0, into(sendd, q))
    for q in range(2):
        remote(sendd.at[q], got0.at[pair], dsend, drecv, block_of + 2 * far_chip + q).start()

    pltpu.make_async_copy(kv_w, kv_w, wsem.at[3]).wait()

    def kv_pack(x, owner, buffer):
        base = base_of(owner, fold1, stride1, 2)
        parts = [dot(x, kv_w[:, i * width : (i + 1) * width]) for i in range(2)]
        for p in range(PAIRS):
            pack(parts, p, p * LANE, base, fold1, stride1, into(buffer, p))

    def spread(buffer, got, send, recv, g):
        for j in (2, 3, 6, 7, 4, 5, 1) if g is None else range(PAIRS):
            turn = pair
            for bit in (1, 2, 4):
                if j & bit:
                    turn = flip(turn, bit)
            to = (group if g is None else g) * HEADS + side * PAIRS + turn
            remote(buffer.at[turn], got.at[my_slot], send, recv, to).start()

    if groups > 1:
        kv_pack(modulated, me, send2)

        @pl.loop(1, groups)
        def _(g):
            spread(send2, got2, tsend, trecv, lax.rem(group + g, groups))

    norm_copies[0].wait_recv()
    kv_pack((ngot[...].astype(F32) * gain + shift).astype(BF16), mirror, send1)
    spread(send1, got1, rsend, rrecv, None)
    if groups > 1:

        @pl.loop(1, groups)
        def _(g):
            spread(send1, got1, rsend, rrecv, lax.rem(group + g, groups))

    got1[my_slot] = send1[pair]

    to_odd(gates, gsend, grecv)

    pltpu.make_async_copy(near_w, near_w, wsem.at[2]).wait()
    norm_copies[1].wait_recv()
    norm_copies[2].wait_recv()
    others = [(ref[...].astype(F32) * gain + shift).astype(BF16) for ref in (xgot, zgot)]
    parts = pair_parts(jnp.concatenate([modulated] + others, axis=0), near_w)
    owners = [pair, flip(pair, 2), flip(pair, 4)]
    bases = [base0] + [base_of(block_of + owner, fold0, stride0, 3) for owner in owners[1:]]
    mine = lax.rem(pair, 2)
    for b in range(3):
        own = [part[b * rows : (b + 1) * rows] for part in parts]
        for q in range(2):
            pack(own, 2 * chip + q, q * LANE, bases[b], fold0, stride0, into(sendp, 2 * b + q))
    for b in range(3):
        remote(sendp.at[2 * b + 1 - mine], got0.at[owners[b]], psend, precv, partner).start()
    for b in range(3):
        got0[owners[b]] = sendp[2 * b + mine]

    drain(got0.at[pl.ds(0, 3)], precv)
    drain(got0.at[pl.ds(0, 2)], drecv)

    def keys_of(got, g, first, fold_group, stride, to):
        block = got[pl.ds(g * PAIRS, PAIRS)]
        cells = PAIRS * rows
        k = block[:, first * rows : (first + 1) * rows].reshape(cells, LANE)
        v = block[:, (first + 1) * rows : (first + 2) * rows].reshape(cells, LANE)
        extra = jnp.concatenate(
            [unfold(block[s, (first + 2) * rows :].astype(F32), rows, stride, to) for s in range(PAIRS)],
            axis=0,
        ).astype(BF16)
        lanes = lax.broadcasted_iota(jnp.int32, (cells, LANE), 1)
        copies = jnp.where(lanes < ex, pltpu.roll(extra, LANE - 2 * ex, axis=1), 0.0).astype(BF16)
        step = ex
        while step < LANE:
            copies = copies + pltpu.roll(copies, step, axis=1)
            step *= 2
        return jnp.concatenate([k, extra], axis=1), jnp.concatenate([v, copies], axis=1)

    half = PAIRS // 2
    cells = half * rows
    near = pair // half
    q_lanes = lax.broadcasted_iota(jnp.int32, (cells, LANE), 1)
    column = lax.rem(q_lanes + (LANE - ex * pair), LANE)
    first_head = column < head
    bias_one = jnp.where(q_lanes == 3 * ex + 1, 1.0, 0.0)

    def queries_of(base):
        block = got0[pl.ds(base, half)]
        qa = block[:, :rows].reshape(cells, LANE).astype(F32)
        extra = jnp.concatenate(
            [
                unfold(block[s, 3 * rows :].astype(F32), rows, stride0, ex)
                for s in range(half)
            ],
            axis=0,
        )
        extra = jnp.where((q_lanes >= ex) & (q_lanes < 2 * ex), extra, bias_one)
        top = jnp.concatenate([jnp.where(first_head, qa, 0.0), bias_one], axis=1)
        low = jnp.concatenate([jnp.where(first_head, 0.0, qa), extra], axis=1)
        return jnp.concatenate([top, low], axis=0).astype(BF16)

    starts = [(1 - near) * half, near * half]
    queries = [queries_of(base) for base in starts]

    def wide(x, count):
        return jnp.concatenate([x] * count, axis=1)

    def attend(i, keys, values, first):
        scores = dot_t(queries[i], keys)
        shape = (scores.shape[0], LANE)
        top = jnp.broadcast_to(jnp.max(scores, axis=1, keepdims=True), shape)
        if not first:
            before = top_s[i]
            top = jnp.maximum(top, before)
        prob = jnp.exp2(scores - wide(top, scores.shape[1] // LANE))
        total = jnp.broadcast_to(jnp.sum(prob, axis=1, keepdims=True), shape)
        mixed = dot(prob.astype(BF16), values)
        if not first:
            decay = jnp.exp2(before - top)
            total = total_s[i] * decay + total
            mixed = o_s[i] * wide(decay, 2) + mixed
        return top, total, mixed

    def keep(i, state):
        top_s[i], total_s[i], o_s[i] = state

    keys, values = keys_of(got0, 0, 1, fold0, stride0, 0)
    for i in range(2):
        keep(i, attend(i, keys, values, True))

    if groups > 1:
        drain(got2.at[pl.ds(0, slots - PAIRS)], trecv)
    drain(got1.at[pl.ds(0, slots - 1)], rrecv)
    for g in range(1, groups):
        other = lax.rem(group + g, groups)
        for got in (got1, got2):
            keys, values = keys_of(got, other, 0, fold1, stride1, ex)
            for i in range(2):
                keep(i, attend(i, keys, values, False))

    keys, values = keys_of(got1, group, 0, fold1, stride1, ex)
    fold_zero = jnp.zeros((fold2, LANE), F32)
    fold_lanes = lax.broadcasted_iota(jnp.int32, (fold2, LANE), 1)
    scores = [dot_t(query, keys) for query in queries]
    finals = []
    for i in range(2):
        shape = (scores[i].shape[0], LANE)
        top = jnp.broadcast_to(jnp.max(scores[i], axis=1, keepdims=True), shape)
        top = jnp.maximum(top, top_s[i])
        prob = jnp.exp2(scores[i] - wide(top, scores[i].shape[1] // LANE))
        total = jnp.broadcast_to(jnp.sum(prob, axis=1, keepdims=True), shape)
        decay = jnp.exp2(top_s[i] - top)
        share = 1.0 / (total_s[i] * decay + total)
        finals.append((prob.astype(BF16), decay * share, share))
    for i in range(2):
        prob, old, new = finals[i]
        mixed = o_s[i] * wide(old, 2) + dot(prob, values) * wide(new, 2)
        main = jnp.where(first_head, mixed[:cells, :LANE], mixed[cells:, :LANE])
        extra = mixed[cells:, LANE:]
        for s in range(half):
            span_s = slice(s * rows, (s + 1) * rows)
            slot = starts[i] + s
            att[slot, :rows, :] = main[span_s].astype(BF16)
            packed = fold_zero
            for r in range(rows // fold2):
                low = s * rows + r * fold2
                packed = jnp.where(
                    (fold_lanes >= r * ex) & (fold_lanes < (r + 1) * ex), extra[low : low + fold2], packed
                )
            att[slot, rows:, :] = packed.astype(BF16)
        for j in (6, 7, 4, 5) if i == 0 else (2, 3, 1):
            slot = pair
            for bit in (1, 2, 4):
                if j & bit:
                    slot = flip(slot, bit)
            remote(att.at[slot], back.at[pair], asend, arecv, me - pair + slot).start()

    total_of(gates, gsum, grecv, fsend, frecv)
    back[pair] = att[pair]
    ow_load.wait()
    valid = (lax.broadcasted_iota(jnp.int32, (rows, 1), 0) < counts[me]).astype(F32)

    sent(mods, msend)
    sent(gates, gsend)

    @pl.when(core == 1)
    def _():
        drain(msum, hsend)

    for copy in norm_copies:
        copy.wait_send()
    drain(got0.at[pl.ds(0, 2)], dsend)
    drain(got0.at[pl.ds(0, 3)], psend)
    if groups > 1:
        drain(got2.at[pl.ds(0, slots - PAIRS)], tsend)
    drain(got1.at[pl.ds(0, slots - 1)], rsend)
    drain(back.at[pl.ds(0, PAIRS - 1)], arecv)


    @pl.when(core == 1)
    def _():
        drain(gsum, fsend)

    @pl.when(core == 0)
    def _():
        drain(gsum, frecv)

    gate_rows = gsum[...]
    gate = jnp.concatenate([gate_rows[0:1], gate_rows[1:2, 2 * span - width :]], axis=1)
    rest = jnp.zeros((rows, LANE), F32)
    for p in range(PAIRS):
        piece = unfold(back[p, rows:, :].astype(F32), rows, ex, p * ex)
        rest = jnp.where((lane_ids >= p * ex) & (lane_ids < (p + 1) * ex), piece, rest)
    chunks = []
    for c in range(PAIRS + 1):
        here = back[c, :rows, :].astype(F32) if c < PAIRS else rest
        if c:
            here = jnp.where(lane_ids < c * ex, rest, here)
            here = jnp.where(lane_ids < (c - 1) * ex, back[c - 1, :rows, :].astype(F32), here)
        chunks.append(here)
    attended = jnp.concatenate(chunks, axis=1).astype(BF16)
    projected = dot(attended, ow[...])
    out[...] = (xin_s[...] + gate * projected * valid).astype(BF16)
    drain(back.at[pl.ds(0, PAIRS - 1)], asend)


def tables(width, freq):
    quarter, half = width // 4, freq // 2
    omega = np.power(10000.0, -np.arange(quarter) / quarter)
    turn = math.pi / 2
    pos_tab = np.stack([np.tile(omega, 4), np.repeat([0.0, turn, 0.0, turn], quarter)])
    wave = np.exp(-math.log(10000.0) * np.arange(half) / half)
    time_tab = np.stack([np.tile(wave, 2), np.repeat([turn, 0.0], half)])
    return pos_tab.astype(np.float32), time_tab.astype(np.float32)


def per_device(
    tokens, positions, counts, timestep, time_in, time_out, ada_weight, qkv_weight, out_weight
):
    n = lax.axis_size("patch")
    rows, width = tokens.shape
    head = width // HEADS
    ex = 2 * head - LANE
    assert 0 < ex and PAIRS * ex <= LANE and n % HEADS == 0
    size0 = 3 * rows + fold_rows(rows, 3 * ex + 2)
    size1 = 2 * rows + fold_rows(rows, 2 * ex + 2)
    size2 = rows + fold_rows(rows, ex)
    slots = n // 2
    queries = PAIRS * rows
    span = -(-width // 256) * LANE
    pos_tab, time_tab = tables(width, time_in.shape[0])
    hbm = pl.BlockSpec(memory_space=pl.ANY)
    vmem = pl.BlockSpec(memory_space=pltpu.VMEM)
    dma = pltpu.SemaphoreType.DMA
    return pl.pallas_call(
        functools.partial(block_kernel, n, rows, width, head),
        out_shape=pltpu.VMEM((rows, width), BF16),
        in_specs=[hbm] * 11,
        out_specs=vmem,
        scratch_shapes=[
            pltpu.SMEM(counts.shape, jnp.int32),
            pltpu.SMEM(timestep.shape, jnp.int32),
            pltpu.VMEM(positions.shape, jnp.int32),
            pltpu.VMEM(pos_tab.shape, F32),
            pltpu.VMEM(time_tab.shape, F32),
            pltpu.VMEM(tokens.shape, BF16),
            pltpu.VMEM(time_in.shape, BF16),
            pltpu.VMEM(time_out.shape[::-1], BF16),
            pltpu.VMEM(ada_weight.shape, BF16),
            pltpu.VMEM((width, 9 * LANE), BF16),
            pltpu.VMEM((width, 9 * LANE), BF16),
            pltpu.VMEM((width, 2 * width), BF16),
            pltpu.VMEM(out_weight.shape, BF16),
            pltpu.VMEM((n, 2, width), BF16),
            pltpu.VMEM((n, 2, span), BF16),
            pltpu.VMEM((2, width), F32),
            pltpu.VMEM((2, span), F32),
            pltpu.VMEM((rows, width), F32),
            pltpu.VMEM((rows, width), F32),
            pltpu.VMEM((rows, width), BF16),
            pltpu.VMEM((rows, width), BF16),
            pltpu.VMEM((rows, width), BF16),
            pltpu.VMEM((rows, width), BF16),
            pltpu.VMEM((2, size0, LANE), BF16),
            pltpu.VMEM((6, size0, LANE), BF16),
            pltpu.VMEM((PAIRS, size1, LANE), BF16),
            pltpu.VMEM((PAIRS, size1, LANE), BF16),
            pltpu.VMEM((PAIRS, size0, LANE), BF16),
            pltpu.VMEM((slots, size1, LANE), BF16),
            pltpu.VMEM((slots, size1, LANE), BF16),
            pltpu.VMEM((2, queries, 2 * LANE), F32),
            pltpu.VMEM((2, queries, LANE), F32),
            pltpu.VMEM((2, queries, LANE), F32),
            pltpu.VMEM((PAIRS, size2, LANE), BF16),
            pltpu.VMEM((PAIRS, size2, LANE), BF16),
            dma((5,)),
            dma((5,)),
        ]
        + [dma((4,))] + [dma((1,))] * 4 + [dma((3,))] * 2 + [dma((1,))] * 14,
        compiler_params=pltpu.CompilerParams(
            collective_id=0, has_side_effects=True, vmem_limit_bytes=60 * 2**20
        ),
    )(
        counts, timestep, positions, pos_tab, time_tab,
        tokens, time_in, time_out.T, ada_weight, qkv_weight, out_weight,
    )


def solution(mesh):
    placed = (
        P(("req", "patch"), None),
        P(None, ("req", "patch")),
        P("req"),
        P("req"),
        P(),
        P(None, "patch"),
        P("patch", None),
        P(),
        P(),
    )
    return jax.shard_map(
        per_device, mesh=mesh, in_specs=placed, out_specs=P(("req", "patch"), None), check_vma=False
    )
```

```python
import functools
import math

import jax
import jax.numpy as jnp
import numpy as np
from jax import lax
from jax.experimental import pallas as pl
from jax.experimental.pallas import tpu as pltpu
from jax.sharding import PartitionSpec as P

HEADS = 16
PAIRS = HEADS // 2
LANE = 128
NEG = -1e30
F32 = jnp.float32
BF16 = jnp.bfloat16
MESH = pl.DeviceIdType.MESH
PI_PARTS = (3.140625, 0.000967502593994140625, 1.509957990978376432e-07)


def silu(v):
    return v / (1.0 + jnp.exp(-v))


def sine(x):
    turns = jnp.floor(x * (1.0 / math.pi) + 0.5)
    r = x - turns * PI_PARTS[0]
    r = r - turns * PI_PARTS[1]
    r = r - turns * PI_PARTS[2]
    s = r * r
    poly = -2.3889859e-08 * s + 2.7525562e-06
    poly = poly * s - 0.00019840874
    poly = poly * s + 0.0083333310
    poly = poly * s - 0.16666667
    value = r + r * (s * poly)
    odd = turns - 2.0 * jnp.floor(turns * 0.5)
    return value * (1.0 - 2.0 * odd)


def dot(a, b):
    return jnp.dot(a, b, preferred_element_type=F32)


def dot_t(a, b):
    return lax.dot_general(a, b, (((1,), (1,)), ((), ())), preferred_element_type=F32)


def one_row_dot(row, matrix):
    wide = jnp.broadcast_to(row, (16, row.shape[1])).astype(BF16)
    return dot(wide, matrix)[0:1]


def fold_rows(rows, stride):
    group = 8
    while rows % group or rows // group * stride > LANE:
        group += 8
    return group


def turned(x, shift):
    if isinstance(shift, int):
        shift %= LANE
        return pltpu.roll(x, shift, axis=1) if shift else x
    return pltpu.roll(x, lax.rem(shift + LANE, LANE), axis=1)


def flip(index, bit):
    return index + bit * (1 - 2 * lax.rem(index // bit, 2))


def fold(blocks, base, group, stride, ex, at):
    lanes = lax.broadcasted_iota(jnp.int32, (group, LANE), 1)
    packed = base
    for r in range(blocks[0].shape[0] // group):
        for j, block in enumerate(blocks):
            low = r * stride + j * ex
            piece = turned(block[r * group : (r + 1) * group], low - at)
            packed = jnp.where((lanes >= low) & (lanes < low + ex), piece, packed)
    return packed


def unfold(packed, rows, stride, to):
    group = packed.shape[0]
    return jnp.concatenate(
        [turned(packed, to - r * stride) for r in range(rows // group)], axis=0
    )


def block_kernel(
    n, rows, width, head,
    counts_h, tstep_h, pos_h, pos_tab_h, time_tab_h,
    tok_h, tin_h, tout_h, ada_h, qkv_h, ow_h,
    out,
    counts, tstep, pos, pos_tab, time_tab, tok, tin, tout, ada, near_w, far_w, kv_w, ow,
    mods, gates, msum, gsum, xin_s, norm_s, nsend, ngot, xgot, zgot, sendd, sendp, send1, send2,
    got0, got1, got2, o_s, top_s, total_s, att, back,
    lsem, ssem, wsem, msend, mrecv, gsend, grecv, nsem, nrecv, dsend, drecv, psend, precv,
    rsend, rrecv, tsend, trecv, asend, arecv, hsend, hrecv, fsend, frecv,
):
    me = lax.axis_index("patch")
    pair = lax.rem(me, PAIRS)
    side = lax.rem(me // PAIRS, 2)
    group = me // HEADS
    groups = n // HEADS
    mirror = flip(flip(me, PAIRS), PAIRS // 2)
    ex = 2 * head - LANE
    stride0, stride1 = 3 * ex + 2, 2 * ex + 2
    fold0, fold1, fold2 = fold_rows(rows, stride0), fold_rows(rows, stride1), fold_rows(rows, ex)
    scale_q = math.log2(math.e) / math.sqrt(head)

    barrier = pltpu.get_barrier_semaphore()

    def drain(ref, sem):
        pltpu.make_async_copy(ref, ref, sem.at[0]).wait()

    def remote(src, dst, send, recv, to):
        return pltpu.make_async_remote_copy(
            src_ref=src, dst_ref=dst, send_sem=send.at[0], recv_sem=recv.at[0],
            device_id={"patch": to}, device_id_type=MESH,
        )

    def greet(to):
        pl.semaphore_signal(barrier, inc=1, device_id={"patch": to}, device_id_type=MESH)

    loads = [
        pltpu.make_async_copy(src, dst, lsem.at[i])
        for i, (src, dst) in enumerate(
            [(tin_h, tin), (tout_h, tout), (ada_h, ada), (tok_h, tok)]
        )
    ]
    chip = pair // 2
    far_chip = flip(flip(pair, 2), 4) // 2
    reach = near_w.shape[1] // 3

    def window(i, owner):
        return pl.ds(pl.multiple_of(i * width + 2 * LANE * owner, LANE), reach)

    qkv_loads = [
        pltpu.make_async_copy(
            qkv_h.at[:, window(i, owner)], dst.at[:, pl.ds(i * reach, reach)], wsem.at[k]
        )
        for k, (owner, dst) in ((1, (far_chip, far_w)), (2, (chip, near_w)))
        for i in range(3)
    ]
    qkv_loads.insert(3, pltpu.make_async_copy(qkv_h.at[:, pl.ds(width, 2 * width)], kv_w, wsem.at[3]))
    small = [
        pltpu.make_async_copy(src, dst, ssem.at[i])
        for i, (src, dst) in enumerate(
            [(tstep_h, tstep), (time_tab_h, time_tab), (counts_h, counts),
             (pos_h, pos), (pos_tab_h, pos_tab)]
        )
    ]
    for load in small[2:] + loads[3:] + small[:2] + loads[:3]:
        load.start()

    @pl.when(lax.rem(me, 2) == 1)
    def _():
        @pl.loop(1, n)
        def _(step):
            greet(lax.rem(me + step, n))

    @pl.when(lax.rem(me, 2) == 0)
    def _():
        greet(mirror)

        @pl.loop(1, n // 2)
        def _(step):
            turn = lax.rem(me // HEADS * PAIRS + pair + step, n // 2)
            greet(turn // PAIRS * HEADS + side * PAIRS + lax.rem(turn, PAIRS))


    ids = lax.broadcasted_iota(jnp.int32, (rows, rows), 0)
    eye = ids == lax.broadcasted_iota(jnp.int32, (rows, rows), 1)
    for load in small[2:]:
        load.wait()
    posf = pos[...].astype(F32)
    row_col = jnp.sum(jnp.where(eye, posf[0:1, :], 0.0), axis=1, keepdims=True)
    col_col = jnp.sum(jnp.where(eye, posf[1:2, :], 0.0), axis=1, keepdims=True)
    wide_lanes = lax.broadcasted_iota(jnp.int32, (1, width), 1)
    place = jnp.where(wide_lanes < width // 2, row_col, col_col)
    embed = sine(place * pos_tab[0:1, :] + pos_tab[1:2, :])
    loads[3].wait()
    x_in = tok[...].astype(F32) + embed
    xin_s[...] = x_in
    centered = x_in - jnp.mean(x_in, axis=1, keepdims=True)
    variance = jnp.mean(centered * centered, axis=1, keepdims=True)
    norm = centered * lax.rsqrt(variance + 1e-6)
    norm_s[...] = norm
    nsend[...] = norm.astype(BF16)
    for load in small[:2]:
        load.wait()
    angles = tstep[0].astype(F32) * time_tab[0:1, :] + time_tab[1:2, :]
    features = sine(angles).astype(BF16)
    loads[0].wait()
    hidden = silu(one_row_dot(features, tin[...])).astype(BF16)
    loads[1].wait()
    wide = jnp.broadcast_to(hidden, (16, width))
    cond = dot_t(wide, tout[...])
    activated = silu(cond[0:1]).astype(BF16)
    loads[2].wait()
    partial = one_row_dot(activated, ada[...])
    mods[me] = jnp.concatenate(
        [partial[:, :width], partial[:, width : 2 * width]], axis=0
    ).astype(BF16)
    span = gates.shape[2]
    gates[me] = jnp.concatenate(
        [partial[:, 2 * width : 2 * width + span], partial[:, 3 * width - span :]], axis=0
    ).astype(BF16)
    for load in qkv_loads:
        load.start()
    ow_load = pltpu.make_async_copy(ow_h, ow, wsem.at[0])
    ow_load.start()


    @pl.when(lax.rem(me, 2) == 1)
    def _():
        pl.semaphore_wait(barrier, n // 4 * 3 - 1)

    @pl.when(lax.rem(me, 2) == 0)
    def _():
        pl.semaphore_wait(barrier, n // 4 * 3)


    core = lax.rem(me, 2)
    partner = flip(me, 1)
    half_n = n // 2

    def to_odd(ref, send, recv):
        @pl.loop(1, half_n)
        def _(step):
            to = 2 * lax.rem(me // 2 + step, half_n) + 1
            remote(ref.at[me], ref.at[me], send, recv, to).start()

        @pl.when(core == 0)
        def _():
            remote(ref.at[me], ref.at[me], send, recv, partner).start()

    def total_of(ref, total, recv, send, done):
        @pl.when(core == 1)
        def _():
            drain(ref.at[pl.ds(0, n - 1)], recv)
            total[...] = jnp.sum(ref[...].astype(F32), axis=0)
            remote(total, total, send, done, partner).start()

    def sent(ref, send):
        @pl.when(core == 0)
        def _():
            drain(ref.at[pl.ds(0, half_n)], send)

        @pl.when(core == 1)
        def _():
            drain(ref.at[pl.ds(0, half_n - 1)], send)

    to_odd(mods, msend, mrecv)

    norm_copies = [
        pltpu.make_async_remote_copy(
            src_ref=nsend, dst_ref=dst, send_sem=nsem.at[i], recv_sem=nrecv.at[i],
            device_id={"patch": to}, device_id_type=MESH,
        )
        for i, (dst, to) in enumerate([(ngot, mirror), (zgot, flip(me, 4)), (xgot, flip(me, 2))])
    ]
    for copy in norm_copies:
        copy.start()

    total_of(mods, msum, mrecv, hsend, hrecv)

    @pl.when(core == 0)
    def _():
        drain(msum, hrecv)

    modulation = msum[...]
    shift = modulation[0:1]
    gain = 1.0 + modulation[1:2]
    modulated = (norm_s[...] * gain + shift).astype(BF16)

    lane_ids = lax.broadcasted_iota(jnp.int32, (rows, LANE), 1)

    def base_of(owner, fold_group, stride, blocks):
        lanes = lax.broadcasted_iota(jnp.int32, (fold_group, LANE), 1)
        slot = lax.broadcasted_iota(jnp.int32, (fold_group, LANE), 0)
        base = jnp.zeros((fold_group, LANE), F32)
        for r in range(rows // fold_group):
            low = r * stride + blocks * ex
            base = jnp.where(lanes == low, 1.0, base)
            bias = jnp.where(slot + r * fold_group < counts[owner], 0.0, NEG)
            base = jnp.where(lanes == low + 1, bias, base)
        return base

    def pack(parts, p, low, base, fold_group, stride, write):
        cut = p * ex
        nexts = []
        for j, part in enumerate(parts):
            here = part[:, low : low + LANE]
            after = part[:, low + LANE : low + 2 * LANE]
            nexts.append(after)
            mixed = jnp.where(lane_ids < cut, after, here)
            write(slice(j * rows, (j + 1) * rows), mixed.astype(BF16))
        packed = fold(nexts, base, fold_group, stride, ex, cut)
        write(slice(len(parts) * rows, None), packed.astype(BF16))

    def into(ref, index):
        def write(part, value):
            ref[index, part, :] = value

        return write

    def pair_parts(x, weights):
        product = dot(x, weights[...])
        parts = [product[:, i * reach : (i + 1) * reach] for i in range(3)]
        return [parts[0] * scale_q] + parts[1:]

    my_slot = group * PAIRS + pair
    slots = groups * PAIRS
    block_of = me - pair
    pltpu.make_async_copy(far_w, far_w, wsem.at[1]).wait()
    base0 = base_of(me, fold0, stride0, 3)
    parts = pair_parts(modulated, far_w)
    for q in range(2):
        pack(parts, 2 * far_chip + q, q * LANE, base0, fold0, stride0, into(sendd, q))
    for q in range(2):
        remote(sendd.at[q], got0.at[pair], dsend, drecv, block_of + 2 * far_chip + q).start()

    pltpu.make_async_copy(kv_w, kv_w, wsem.at[3]).wait()

    def kv_pack(x, owner, buffer):
        base = base_of(owner, fold1, stride1, 2)
        parts = [dot(x, kv_w[:, i * width : (i + 1) * width]) for i in range(2)]
        for p in range(PAIRS):
            pack(parts, p, p * LANE, base, fold1, stride1, into(buffer, p))

    def spread(buffer, got, send, recv, g):
        for j in (2, 3, 6, 7, 4, 5, 1) if g is None else range(PAIRS):
            turn = pair
            for bit in (1, 2, 4):
                if j & bit:
                    turn = flip(turn, bit)
            to = (group if g is None else g) * HEADS + side * PAIRS + turn
            remote(buffer.at[turn], got.at[my_slot], send, recv, to).start()

    if groups > 1:
        kv_pack(modulated, me, send2)

        @pl.loop(1, groups)
        def _(g):
            spread(send2, got2, tsend, trecv, lax.rem(group + g, groups))

    norm_copies[0].wait_recv()
    kv_pack((ngot[...].astype(F32) * gain + shift).astype(BF16), mirror, send1)
    spread(send1, got1, rsend, rrecv, None)
    if groups > 1:

        @pl.loop(1, groups)
        def _(g):
            spread(send1, got1, rsend, rrecv, lax.rem(group + g, groups))

    got1[my_slot] = send1[pair]


    pltpu.make_async_copy(near_w, near_w, wsem.at[2]).wait()
    norm_copies[1].wait_recv()
    norm_copies[2].wait_recv()
    others = [(ref[...].astype(F32) * gain + shift).astype(BF16) for ref in (xgot, zgot)]
    parts = pair_parts(jnp.concatenate([modulated] + others, axis=0), near_w)
    owners = [pair, flip(pair, 2), flip(pair, 4)]
    bases = [base0] + [base_of(block_of + owner, fold0, stride0, 3) for owner in owners[1:]]
    mine = lax.rem(pair, 2)
    for b in range(3):
        own = [part[b * rows : (b + 1) * rows] for part in parts]
        for q in range(2):
            pack(own, 2 * chip + q, q * LANE, bases[b], fold0, stride0, into(sendp, 2 * b + q))
    for b in range(3):
        remote(sendp.at[2 * b + 1 - mine], got0.at[owners[b]], psend, precv, partner).start()
    for b in range(3):
        got0[owners[b]] = sendp[2 * b + mine]

    to_odd(gates, gsend, grecv)

    drain(got0.at[pl.ds(0, 3)], precv)
    drain(got0.at[pl.ds(0, 2)], drecv)

    def keys_of(got, g, first, fold_group, stride, to):
        block = got[pl.ds(g * PAIRS, PAIRS)]
        cells = PAIRS * rows
        k = block[:, first * rows : (first + 1) * rows].reshape(cells, LANE)
        v = block[:, (first + 1) * rows : (first + 2) * rows].reshape(cells, LANE)
        extra = jnp.concatenate(
            [unfold(block[s, (first + 2) * rows :].astype(F32), rows, stride, to) for s in range(PAIRS)],
            axis=0,
        ).astype(BF16)
        lanes = lax.broadcasted_iota(jnp.int32, (cells, LANE), 1)
        copies = jnp.where(lanes < ex, pltpu.roll(extra, LANE - 2 * ex, axis=1), 0.0).astype(BF16)
        step = ex
        while step < LANE:
            copies = copies + pltpu.roll(copies, step, axis=1)
            step *= 2
        return jnp.concatenate([k, extra], axis=1), jnp.concatenate([v, copies], axis=1)

    half = PAIRS // 2
    cells = half * rows
    near = pair // half
    q_lanes = lax.broadcasted_iota(jnp.int32, (cells, LANE), 1)
    column = lax.rem(q_lanes + (LANE - ex * pair), LANE)
    first_head = column < head
    bias_one = jnp.where(q_lanes == 3 * ex + 1, 1.0, 0.0)

    def queries_of(base):
        block = got0[pl.ds(base, half)]
        qa = block[:, :rows].reshape(cells, LANE).astype(F32)
        extra = jnp.concatenate(
            [
                unfold(block[s, 3 * rows :].astype(F32), rows, stride0, ex)
                for s in range(half)
            ],
            axis=0,
        )
        extra = jnp.where((q_lanes >= ex) & (q_lanes < 2 * ex), extra, bias_one)
        top = jnp.concatenate([jnp.where(first_head, qa, 0.0), bias_one], axis=1)
        low = jnp.concatenate([jnp.where(first_head, 0.0, qa), extra], axis=1)
        return jnp.concatenate([top, low], axis=0).astype(BF16)

    starts = [(1 - near) * half, near * half]
    queries = [queries_of(base) for base in starts]

    def wide(x, count):
        return jnp.concatenate([x] * count, axis=1)

    def attend(i, keys, values, first):
        scores = dot_t(queries[i], keys)
        shape = (scores.shape[0], LANE)
        top = jnp.broadcast_to(jnp.max(scores, axis=1, keepdims=True), shape)
        if not first:
            before = top_s[i]
            top = jnp.maximum(top, before)
        prob = jnp.exp2(scores - wide(top, scores.shape[1] // LANE))
        total = jnp.broadcast_to(jnp.sum(prob, axis=1, keepdims=True), shape)
        mixed = dot(prob.astype(BF16), values)
        if not first:
            decay = jnp.exp2(before - top)
            total = total_s[i] * decay + total
            mixed = o_s[i] * wide(decay, 2) + mixed
        return top, total, mixed

    def keep(i, state):
        top_s[i], total_s[i], o_s[i] = state

    keys, values = keys_of(got0, 0, 1, fold0, stride0, 0)
    for i in range(2):
        keep(i, attend(i, keys, values, True))

    if groups > 1:
        drain(got2.at[pl.ds(0, slots - PAIRS)], trecv)
    drain(got1.at[pl.ds(0, slots - 1)], rrecv)
    for g in range(1, groups):
        other = lax.rem(group + g, groups)
        for got in (got1, got2):
            keys, values = keys_of(got, other, 0, fold1, stride1, ex)
            for i in range(2):
                keep(i, attend(i, keys, values, False))

    keys, values = keys_of(got1, group, 0, fold1, stride1, ex)
    fold_zero = jnp.zeros((fold2, LANE), F32)
    fold_lanes = lax.broadcasted_iota(jnp.int32, (fold2, LANE), 1)
    for i in range(2):
        scores = dot_t(queries[i], keys)
        shape = (scores.shape[0], LANE)
        top = jnp.broadcast_to(jnp.max(scores, axis=1, keepdims=True), shape)
        top = jnp.maximum(top, top_s[i])
        prob = jnp.exp2(scores - wide(top, scores.shape[1] // LANE))
        total = jnp.broadcast_to(jnp.sum(prob, axis=1, keepdims=True), shape)
        decay = jnp.exp2(top_s[i] - top)
        share = 1.0 / (total_s[i] * decay + total)
        mixed = o_s[i] * wide(decay * share, 2) + dot(prob.astype(BF16), values) * wide(share, 2)
        main = jnp.where(first_head, mixed[:cells, :LANE], mixed[cells:, :LANE])
        extra = mixed[cells:, LANE:]
        for s in range(half):
            span_s = slice(s * rows, (s + 1) * rows)
            slot = starts[i] + s
            att[slot, :rows, :] = main[span_s].astype(BF16)
            packed = fold_zero
            for r in range(rows // fold2):
                low = s * rows + r * fold2
                packed = jnp.where(
                    (fold_lanes >= r * ex) & (fold_lanes < (r + 1) * ex), extra[low : low + fold2], packed
                )
            att[slot, rows:, :] = packed.astype(BF16)
        for j in (6, 7, 4, 5) if i == 0 else (2, 3, 1):
            slot = pair
            for bit in (1, 2, 4):
                if j & bit:
                    slot = flip(slot, bit)
            remote(att.at[slot], back.at[pair], asend, arecv, me - pair + slot).start()

    total_of(gates, gsum, grecv, fsend, frecv)
    back[pair] = att[pair]
    ow_load.wait()
    valid = (lax.broadcasted_iota(jnp.int32, (rows, 1), 0) < counts[me]).astype(F32)

    sent(mods, msend)
    sent(gates, gsend)

    @pl.when(core == 1)
    def _():
        drain(msum, hsend)

    for copy in norm_copies:
        copy.wait_send()
    drain(got0.at[pl.ds(0, 2)], dsend)
    drain(got0.at[pl.ds(0, 3)], psend)
    if groups > 1:
        drain(got2.at[pl.ds(0, slots - PAIRS)], tsend)
    drain(got1.at[pl.ds(0, slots - 1)], rsend)
    drain(back.at[pl.ds(0, PAIRS - 1)], arecv)


    @pl.when(core == 1)
    def _():
        drain(gsum, fsend)

    @pl.when(core == 0)
    def _():
        drain(gsum, frecv)

    gate_rows = gsum[...]
    gate = jnp.concatenate([gate_rows[0:1], gate_rows[1:2, 2 * span - width :]], axis=1)
    rest = jnp.zeros((rows, LANE), F32)
    for p in range(PAIRS):
        piece = unfold(back[p, rows:, :].astype(F32), rows, ex, p * ex)
        rest = jnp.where((lane_ids >= p * ex) & (lane_ids < (p + 1) * ex), piece, rest)
    chunks = []
    for c in range(PAIRS + 1):
        here = back[c, :rows, :].astype(F32) if c < PAIRS else rest
        if c:
            here = jnp.where(lane_ids < c * ex, rest, here)
            here = jnp.where(lane_ids < (c - 1) * ex, back[c - 1, :rows, :].astype(F32), here)
        chunks.append(here)
    attended = jnp.concatenate(chunks, axis=1).astype(BF16)
    projected = dot(attended, ow[...])
    out[...] = (xin_s[...] + gate * projected * valid).astype(BF16)
    drain(back.at[pl.ds(0, PAIRS - 1)], asend)


def tables(width, freq):
    quarter, half = width // 4, freq // 2
    omega = np.power(10000.0, -np.arange(quarter) / quarter)
    turn = math.pi / 2
    pos_tab = np.stack([np.tile(omega, 4), np.repeat([0.0, turn, 0.0, turn], quarter)])
    wave = np.exp(-math.log(10000.0) * np.arange(half) / half)
    time_tab = np.stack([np.tile(wave, 2), np.repeat([turn, 0.0], half)])
    return pos_tab.astype(np.float32), time_tab.astype(np.float32)


def per_device(
    tokens, positions, counts, timestep, time_in, time_out, ada_weight, qkv_weight, out_weight
):
    n = lax.axis_size("patch")
    rows, width = tokens.shape
    head = width // HEADS
    ex = 2 * head - LANE
    assert 0 < ex and PAIRS * ex <= LANE and n % HEADS == 0
    size0 = 3 * rows + fold_rows(rows, 3 * ex + 2)
    size1 = 2 * rows + fold_rows(rows, 2 * ex + 2)
    size2 = rows + fold_rows(rows, ex)
    slots = n // 2
    queries = PAIRS * rows
    span = -(-width // 256) * LANE
    pos_tab, time_tab = tables(width, time_in.shape[0])
    hbm = pl.BlockSpec(memory_space=pl.ANY)
    vmem = pl.BlockSpec(memory_space=pltpu.VMEM)
    dma = pltpu.SemaphoreType.DMA
    return pl.pallas_call(
        functools.partial(block_kernel, n, rows, width, head),
        out_shape=pltpu.VMEM((rows, width), BF16),
        in_specs=[hbm] * 11,
        out_specs=vmem,
        scratch_shapes=[
            pltpu.SMEM(counts.shape, jnp.int32),
            pltpu.SMEM(timestep.shape, jnp.int32),
            pltpu.VMEM(positions.shape, jnp.int32),
            pltpu.VMEM(pos_tab.shape, F32),
            pltpu.VMEM(time_tab.shape, F32),
            pltpu.VMEM(tokens.shape, BF16),
            pltpu.VMEM(time_in.shape, BF16),
            pltpu.VMEM(time_out.shape[::-1], BF16),
            pltpu.VMEM(ada_weight.shape, BF16),
            pltpu.VMEM((width, 9 * LANE), BF16),
            pltpu.VMEM((width, 9 * LANE), BF16),
            pltpu.VMEM((width, 2 * width), BF16),
            pltpu.VMEM(out_weight.shape, BF16),
            pltpu.VMEM((n, 2, width), BF16),
            pltpu.VMEM((n, 2, span), BF16),
            pltpu.VMEM((2, width), F32),
            pltpu.VMEM((2, span), F32),
            pltpu.VMEM((rows, width), F32),
            pltpu.VMEM((rows, width), F32),
            pltpu.VMEM((rows, width), BF16),
            pltpu.VMEM((rows, width), BF16),
            pltpu.VMEM((rows, width), BF16),
            pltpu.VMEM((rows, width), BF16),
            pltpu.VMEM((2, size0, LANE), BF16),
            pltpu.VMEM((6, size0, LANE), BF16),
            pltpu.VMEM((PAIRS, size1, LANE), BF16),
            pltpu.VMEM((PAIRS, size1, LANE), BF16),
            pltpu.VMEM((PAIRS, size0, LANE), BF16),
            pltpu.VMEM((slots, size1, LANE), BF16),
            pltpu.VMEM((slots, size1, LANE), BF16),
            pltpu.VMEM((2, queries, 2 * LANE), F32),
            pltpu.VMEM((2, queries, LANE), F32),
            pltpu.VMEM((2, queries, LANE), F32),
            pltpu.VMEM((PAIRS, size2, LANE), BF16),
            pltpu.VMEM((PAIRS, size2, LANE), BF16),
            dma((5,)),
            dma((5,)),
        ]
        + [dma((4,))] + [dma((1,))] * 4 + [dma((3,))] * 2 + [dma((1,))] * 14,
        compiler_params=pltpu.CompilerParams(
            collective_id=0, has_side_effects=True, vmem_limit_bytes=60 * 2**20
        ),
    )(
        counts, timestep, positions, pos_tab, time_tab,
        tokens, time_in, time_out.T, ada_weight, qkv_weight, out_weight,
    )


def solution(mesh):
    placed = (
        P(("req", "patch"), None),
        P(None, ("req", "patch")),
        P("req"),
        P("req"),
        P(),
        P(None, "patch"),
        P("patch", None),
        P(),
        P(),
    )
    return jax.shard_map(
        per_device, mesh=mesh, in_specs=placed, out_specs=P(("req", "patch"), None), check_vma=False
    )
```
